256 devices in a mesh: rows: 32 (over x_lo, z, core), cols: 8 (over x_hi, y).
Axes of the slice: x: 4 (x_hi: 2, x_lo: 2; x = x_hi * 2 + x_lo), y: 4, z: 8, core: 2. Of those that a mesh axis runs over, the one named last changes fastest.
Arguments:
- rhs: float32 [65536, 16], P(('rows', 'cols')), may hold values from -6 to 6
- diagonal: float32 [65536], P(('rows', 'cols')), may hold values from 1 to 16
- blocks: float32 [512, 16, 128, 128], P('rows', 'cols'), may hold values from -0.078125 to 0.078125
- block_cols: int32 [512, 16], P('rows', 'cols'), may hold values from 0 to 63
- counts: int32 [512, 8], P('rows', 'cols'), may hold values from 1 to 2
Outputs:
- solution: float32 [65536, 16], P(('rows', 'cols'))
The draws below stay inside these ranges and needn't reach their ends.
Inputs may be any that keep to these rules, and one draw needn't show every extreme that they name: Every entry of block_cols names a block column within its slot's group, from 0 to 63; entries may repeat within a row. `counts`: every count lies between 1 and 2; the slots past the count in a group hold blocks that are not used.
All inputs are finite; a program needn't handle non-finite values.
Results may differ from the reference program's by a relative error of at most 0.0001.
Values sent between devices are 32-bit elements; how exact they have to be, the bound alone decides.
A program may use at most 64 MiB of HBM per device.

```python
import math
import jax
import jax.numpy as jnp
from jax import lax

BS = 128
S = 16
KC = 2
ITERS = 4
PB = 2
NB = 512
N = 65536
KB = 16
NBC = 64
N_COLS = 8


def plant(result, own_key, least, largest):
    shape = result.shape
    spot = [jax.random.randint(jax.random.fold_in(own_key, axis), (), 0, shape[axis]) for axis in range(len(shape))]
    result = result.at[tuple(spot)].set(least)
    longest = shape.index(max(shape))
    spot[longest] = (spot[longest] + 1) % shape[longest]
    return result.at[tuple(spot)].set(largest)


def level_of(stream_key, dims, shards, smallest, top_value):
    def one(dim, parts):
        draws = jax.random.uniform(jax.random.fold_in(jax.random.fold_in(stream_key, 6), dim), (parts,), jnp.float32, smallest / len(shards), top_value / len(shards))
        return jnp.repeat(jnp.exp(draws), dims[dim] // parts).reshape((-1,) + (1,) * (len(dims) - dim - 1))

    gain = one(*shards[0])
    for cut in shards[1:]:
        gain = gain * one(*cut)
    return gain


def noise(own_key, shape, scale, reach, shards=(), held_as=jnp.bfloat16):
    array = jax.random.normal(own_key, shape, jnp.float32) * scale
    if len(shards) > 0:
        array = level_of(own_key, shape, shards, -0.22, 0.18) * array
    return jnp.clip(array, min=-reach, max=reach).astype(held_as)


def setup_inputs(seed: int = 0) -> dict:
    seeds = jax.random.split(jax.random.key(seed), 6)
    return {
        "rhs": noise(seeds[0], (N, S), 1.0, 6.0, ((0, 256),), jnp.float32),
        "diagonal": jnp.clip(jnp.exp(math.log(16.0) - 2.7725887 * jax.random.uniform(seeds[1], (N,), jnp.float32) ** level_of(seeds[1], (N,), ((0, 256),), -0.2, 0.2)), 1.0, 16.0),
        "blocks": noise(seeds[2], (NB, KB, BS, BS), (3 * BS * KB) ** -0.5, 0.078125, ((0, 32), (1, 8)), jnp.float32),
        "block_cols": plant(jax.random.randint(seeds[3], (NB, KB), 0, NBC), jax.random.fold_in(seeds[3], 1), 0, NBC - 1).astype(jnp.int32),
        "counts": plant(jax.random.randint(seeds[4], (NB, N_COLS), 1, KC + 1), jax.random.fold_in(seeds[4], 1), 1, KC).astype(jnp.int32),
    }


def solve_block(matrix, right):
    size = matrix.shape[0]
    joined = jnp.concatenate([matrix, right], axis=1)
    for index in range(size):
        pivot_row = joined[index] / joined[index, index]
        joined = joined - joined[:, index:index + 1] * pivot_row[None, :]
        joined = joined.at[index].set(pivot_row)
    return joined[:, size:]


def gram(left, right):
    return jnp.dot(left.T, right, precision=lax.Precision.HIGHEST)


def times_block(vectors, small):
    return jnp.dot(vectors, small, precision=lax.Precision.HIGHEST)


def reference(rhs, diagonal, blocks, block_cols, counts):
    slot = jnp.arange(KB, dtype=jnp.int32)
    group = slot // KC
    within = slot % KC
    used = (within[None, :] < counts[:, group]).astype(jnp.float32)
    target = (block_cols // PB) * (N_COLS * PB) + group[None, :] * PB + block_cols % PB
    target = target.astype(jnp.int32)

    def apply(vectors):
        tiles = vectors.reshape(NB, BS, S)
        picked = tiles[target] * used[:, :, None, None]
        product = jnp.einsum("bkij,bkjs->bis", blocks, picked, precision=lax.Precision.HIGHEST)
        return diagonal[:, None] * vectors + product.reshape(N, S)

    solution = jnp.zeros_like(rhs)
    residual = rhs
    direction = rhs
    shadow = rhs
    for iteration in range(ITERS):
        image = apply(direction)
        matrix = gram(shadow, image)
        right = gram(shadow, residual)
        alpha = solve_block(matrix, right)
        middle = residual - times_block(image, alpha)
        second = apply(middle)
        omega = jnp.sum(second * middle) / jnp.sum(second * second)
        cross = gram(shadow, second)
        solution = solution + times_block(direction, alpha) + omega * middle
        residual = middle - omega * second
        beta = -solve_block(matrix, cross)
        direction = residual + times_block(direction - omega * image, beta)
    return solution
```

```python
import functools

import jax
import jax.numpy as jnp
from jax import lax
from jax.experimental import pallas as pl
from jax.experimental.pallas import tpu as pltpu
from jax.sharding import PartitionSpec as P

ITERS = 4
MESH = pl.DeviceIdType.MESH
HIGHEST = lax.Precision.HIGHEST
F32 = jnp.float32
BF16 = jnp.bfloat16
NT = (((1,), (1,)), ((), ()))
NN = (((1,), (0,)), ((), ()))


def mm(a, b, dims=NN):
    return lax.dot_general(a, b, dims, precision=HIGHEST, preferred_element_type=F32)


def kernel(
    sizes,
    cols_ref, counts_ref, rhs_ref, diag_ref, blocks_ref, out_ref,
    at, gb0, gb1, prod, rsb, arx, ary, arz,
    sh, pv, sv, zv, vv, rv, wv, tv, qv, xv, at_small,
    ag_ssem, ag_rsem, dd_ssem, dd_rsem, rs_ssem, rs_rsem,
    ax_ssem, ax_rsem, ay_ssem, ay_rsem, az_ssem, az_rsem,
):
    NZ, NY = sizes
    r = lax.axis_index("rows")
    c = lax.axis_index("cols")
    core = lax.rem(r, 2)
    z = lax.rem(lax.div(r, 2), NZ)
    a = lax.div(r, 2 * NZ)
    xh = lax.div(c, NY)
    y = lax.rem(c, NY)
    x = xh * 2 + a
    n_cols = 2 * NY

    def row_of(a_, z_, k_):
        return (a_ * NZ + z_) * 2 + k_

    def place(k_, a_, z_):
        return ((k_ * 2 + a_) * NZ + z_) * 2

    z_order = sorted(range(NZ), key=lambda d: -min(d, NZ - d))
    y_order = sorted(range(NY), key=lambda d: -min(d, NY - d))
    gather_peers = []
    for da in (1, 0):
        for dz in z_order:
            if (da, dz) != (0, 0):
                gather_peers.append((lax.rem(a + da, 2), lax.rem(z + dz, NZ)))
    scatter_peers = []
    for dx in (1, 0):
        for dy in y_order:
            if (dx, dy) != (0, 0):
                scatter_peers.append((lax.rem(xh + dx, 2), lax.rem(y + dy, NY)))
    partner = r + 1 - 2 * core
    plane_peers = []
    for dx in (2, 1, 3, 0):
        for dk in (1, 0):
            if (dx, dk) != (0, 0):
                plane_peers.append((lax.rem(x + dx, 4), lax.rem(core + dk, 2)))
    y_peers = [lax.rem(y + d, NY) for d in y_order if d != 0]
    z_peers = [lax.rem(z + d, NZ) for d in z_order if d != 0]

    def plane_device(x_, k_):
        return (row_of(lax.rem(x_, 2), z, k_), lax.div(x_, 2) * NY + y)

    barrier = pltpu.get_barrier_semaphore()
    greet = [(row_of(a_, z_, core), c) for a_, z_ in gather_peers]
    greet.append((partner, c))
    greet += [(r, xh_ * NY + y_) for xh_, y_ in scatter_peers]
    extra = []
    for dx in (2, 1, 3, 0):
        for dk in (1, 0):
            if (dx, dk) in ((0, 0), (2, 0), (0, 1)):
                continue
            extra.append(plane_device(lax.rem(x + dx, 4), lax.rem(core + dk, 2)))
    greet += extra
    for device in greet:
        pl.semaphore_signal(barrier, inc=1, device_id=device, device_id_type=MESH)

    def prepare(b, carry):
        cnt = counts_ref[b]
        for k in range(2):
            blk = blocks_ref[b, k]
            blk = jnp.where(k < cnt, blk, 0.0).T
            hi = blk.astype(BF16)
            mid = (blk - hi.astype(F32)).astype(BF16)
            at[b, k * 128:(k + 1) * 128, 0:128] = hi
            at[b, k * 128:(k + 1) * 128, 128:256] = mid
        return carry

    lax.fori_loop(0, 16, prepare, 0)

    rhs = rhs_ref[...]
    sh[...] = rhs
    rv[...] = rhs
    wv[...] = rhs
    zv[...] = rhs
    qv[...] = rhs
    xv[...] = -rhs
    zero = jnp.zeros_like(rhs)
    pv[...] = zero
    sv[...] = zero
    vv[...] = zero
    tv[...] = zero
    row16 = lax.broadcasted_iota(jnp.int32, (16, 128), 0)
    lane16 = lax.broadcasted_iota(jnp.int32, (16, 128), 1)
    eye_at_32 = jnp.where(lane16 == row16 + 32, 1.0, 0.0)
    row32 = lax.broadcasted_iota(jnp.int32, (32, 128), 0)
    lane32 = lax.broadcasted_iota(jnp.int32, (32, 128), 1)
    pick = jnp.where(lane32 == row32 + 16, 1.0, 0.0)
    pad96 = jnp.zeros((96, 256), F32)
    pad112 = jnp.zeros((112, 256), F32)
    at_small[...] = jnp.zeros((32, 16), F32)

    pl.semaphore_wait(barrier, len(greet))

    gbs = (gb0, gb1)

    def gather_start(par, vec):
        gb = gbs[par]
        mine = place(core, a, z)
        gb[mine] = vec[:, 0:128]
        gb[mine + 1] = vec[:, 128:256]
        sends = []
        for n, (a_, z_) in enumerate(gather_peers):
            cp = pltpu.make_async_remote_copy(
                src_ref=gb.at[pl.ds(mine, 2)],
                dst_ref=gb.at[pl.ds(mine, 2)],
                send_sem=ag_ssem.at[n],
                recv_sem=ag_rsem.at[par, a * NZ + z],
                device_id=(row_of(a_, z_, core), c),
                device_id_type=MESH,
            )
            cp.start()
            sends.append(cp)
        return sends

    def gather_finish(par):
        gb = gbs[par]
        sends = []
        for half in range(2):
            a_half = lax.rem(a + half, 2)
            for dz in reversed(z_order):
                if (half, dz) == (0, 0):
                    continue
                z_ = lax.rem(z + dz, NZ)
                there = place(core, a_half, z_)
                pltpu.make_async_remote_copy(
                    src_ref=gb.at[pl.ds(there, 2)],
                    dst_ref=gb.at[pl.ds(there, 2)],
                    send_sem=ag_ssem.at[0],
                    recv_sem=ag_rsem.at[par, a_half * NZ + z_],
                    device_id=(partner, c),
                    device_id_type=MESH,
                ).wait_recv()
            start = place(core, a_half, 0)
            cp = pltpu.make_async_remote_copy(
                src_ref=gb.at[pl.ds(start, 2 * NZ)],
                dst_ref=gb.at[pl.ds(start, 2 * NZ)],
                send_sem=dd_ssem.at[half],
                recv_sem=dd_rsem.at[par, a_half],
                device_id=(partner, c),
                device_id_type=MESH,
            )
            cp.start()
            sends.append(cp)
        for half in range(2):
            a_half = lax.rem(a + half, 2)
            start = place(1 - core, a_half, 0)
            pltpu.make_async_remote_copy(
                src_ref=gb.at[pl.ds(start, 2 * NZ)],
                dst_ref=gb.at[pl.ds(start, 2 * NZ)],
                send_sem=dd_ssem.at[half],
                recv_sem=dd_rsem.at[par, a_half],
                device_id=(partner, c),
                device_id_type=MESH,
            ).wait_recv()
        return sends

    def block_row(gb, b):
        parts = []
        for k in range(2):
            l = cols_ref[b, k]
            h = l & 1
            k_ = (l >> 1) & 1
            az = l >> 2
            parts.append(gb[((k_ * 2 * NZ + az) << 1) + h])
        v = jnp.concatenate(parts, axis=1)
        vh = v.astype(BF16)
        vm = (v - vh.astype(F32)).astype(BF16)
        both = jnp.concatenate([vh, vm], axis=0)
        full = lax.dot_general(both, at[b], NN, preferred_element_type=F32)
        return full[0:16, 0:128] + (full[16:32, 0:128] + full[0:16, 128:256])

    def products(par):
        gb = gbs[par]
        sends = []
        for n, (xh_, y_) in enumerate(scatter_peers + [(xh, y)]):
            c_ = xh_ * NY + y_
            for h in range(2):
                prod[c_, h] = block_row(gb, c_ * 2 + h)
            if n < len(scatter_peers):
                cp = pltpu.make_async_remote_copy(
                    src_ref=prod.at[c_],
                    dst_ref=rsb.at[par, c],
                    send_sem=rs_ssem.at[n],
                    recv_sem=rs_rsem.at[par, c],
                    device_id=(r, c_),
                    device_id_type=MESH,
                )
                cp.start()
                sends.append(cp)
        return sends

    def scatter_finish(par, vec):
        own = prod[c]
        total = jnp.concatenate([own[0], own[1]], axis=1) + diag_ref[...] * vec
        for xh_, y_ in reversed(scatter_peers):
            c_ = xh_ * NY + y_
            pltpu.make_async_remote_copy(
                src_ref=prod.at[c_],
                dst_ref=rsb.at[par, c_],
                send_sem=rs_ssem.at[0],
                recv_sem=rs_rsem.at[par, c_],
                device_id=(r, c_),
                device_id_type=MESH,
            ).wait_recv()
            got = rsb[par, c_]
            total = total + jnp.concatenate([got[0], got[1]], axis=1)
        return total

    def reduce_x_start(par, part):
        mine = x * 2 + core
        arx[par, mine] = part
        sends = []
        for n, (x_, k_) in enumerate(plane_peers):
            cp = pltpu.make_async_remote_copy(
                src_ref=arx.at[par, mine],
                dst_ref=arx.at[par, mine],
                send_sem=ax_ssem.at[n],
                recv_sem=ax_rsem.at[par, mine],
                device_id=plane_device(x_, k_),
                device_id_type=MESH,
            )
            cp.start()
            sends.append(cp)
        return sends

    def reduce_y_start(par):
        for x_, k_ in reversed(plane_peers):
            slot = x_ * 2 + k_
            pltpu.make_async_remote_copy(
                src_ref=arx.at[par, slot],
                dst_ref=arx.at[par, slot],
                send_sem=ax_ssem.at[0],
                recv_sem=ax_rsem.at[par, slot],
                device_id=plane_device(x_, k_),
                device_id_type=MESH,
            ).wait_recv()
        part = arx[par, 0]
        for s in range(1, 8):
            part = part + arx[par, s]
        ary[par, y] = part
        sends = []
        for n, y_ in enumerate(y_peers):
            cp = pltpu.make_async_remote_copy(
                src_ref=ary.at[par, y],
                dst_ref=ary.at[par, y],
                send_sem=ay_ssem.at[n],
                recv_sem=ay_rsem.at[par, y],
                device_id=(r, xh * NY + y_),
                device_id_type=MESH,
            )
            cp.start()
            sends.append(cp)
        return sends

    def reduce_z_start(par):
        for y_ in reversed(y_peers):
            pltpu.make_async_remote_copy(
                src_ref=ary.at[par, y_],
                dst_ref=ary.at[par, y_],
                send_sem=ay_ssem.at[0],
                recv_sem=ay_rsem.at[par, y_],
                device_id=(r, xh * NY + y_),
                device_id_type=MESH,
            ).wait_recv()
        part = ary[par, 0]
        for s in range(1, NY):
            part = part + ary[par, s]
        arz[par, z] = part
        sends = []
        for n, z_ in enumerate(z_peers):
            cp = pltpu.make_async_remote_copy(
                src_ref=arz.at[par, z],
                dst_ref=arz.at[par, z],
                send_sem=az_ssem.at[n],
                recv_sem=az_rsem.at[par, z],
                device_id=(row_of(a, z_, core), c),
                device_id_type=MESH,
            )
            cp.start()
            sends.append(cp)
        return sends

    def reduce_finish(par):
        for z_ in reversed(z_peers):
            pltpu.make_async_remote_copy(
                src_ref=arz.at[par, z_],
                dst_ref=arz.at[par, z_],
                send_sem=az_ssem.at[0],
                recv_sem=az_rsem.at[par, z_],
                device_id=(row_of(a, z_, core), c),
                device_id_type=MESH,
            ).wait_recv()
        part = arz[par, 0]
        for s in range(1, NZ):
            part = part + arz[par, s]
        return part

    def drain(sends):
        for cp in sends:
            cp.wait_send()

    def omega_part():
        yy = wv[...] - mm(at_small[0:16, :], zv[...])
        return yy

    def sums_of(yy, qq):
        d = mm(yy, jnp.concatenate([sh[...], pad112], axis=0), NT)
        along = jnp.sum(yy * qq, axis=1, keepdims=True)
        square = jnp.sum(yy * yy, axis=1, keepdims=True)
        return jnp.where(lane16 == 16, along, jnp.where(lane16 == 17, square, d))

    def omega_of(total):
        along = jnp.sum(jnp.where(lane16 == 16, total, 0.0), keepdims=True)
        square = jnp.sum(jnp.where(lane16 == 17, total, 0.0), keepdims=True)
        return along / square

    def solve(total):
        joined = jnp.where(lane16 < 32, total, eye_at_32)
        for i in range(16):
            pivot_row = joined[i:i + 1, :] / joined[i:i + 1, i:i + 1]
            column = joined[:, i:i + 1]
            joined = jnp.where(row16 == i, pivot_row, joined - column * pivot_row)
        return mm(pick, joined, NT)

    def step(i, carry):
        first = i == 0
        par = 0
        ag = gather_start(par, zv[...])
        yy = jnp.where(first, 0.0, wv[...] - mm(at_small[0:16, :], zv[...]))
        qq = qv[...]
        ax = reduce_x_start(par, sums_of(yy, qq))
        ay = reduce_y_start(par)
        az = reduce_z_start(par)
        dd = gather_finish(par)
        rs = products(par)
        total = reduce_finish(par)
        omega = jnp.where(first, 1.0, omega_of(total))
        beta_t = jnp.where(first, 0.0, -mm(total[:, 0:16], at_small[16:32, :]))
        alpha_t = at_small[0:16, :]
        xv[...] = xv[...] + mm(alpha_t, pv[...]) + omega * qq
        res = qq - omega * yy
        new_p = res + mm(beta_t, pv[...] - omega * sv[...])
        kept = mm(beta_t, sv[...] - omega * zv[...])
        left = yy - omega * tv[...]
        vv[...] = scatter_finish(par, zv[...])
        w_new = jnp.where(first, vv[...], left + omega * mm(alpha_t, vv[...]))
        drain(ag + ax + ay + az + dd + rs)
        par = 1
        ag = gather_start(par, w_new)
        s_new = w_new + kept
        d = mm(sh[...], jnp.concatenate([s_new, res, pad96], axis=0), NT)
        ax = reduce_x_start(par, d)
        wv[...] = w_new
        pv[...] = new_p
        sv[...] = s_new
        ay = reduce_y_start(par)
        az = reduce_z_start(par)
        dd = gather_finish(par)
        rs = products(par)
        total = reduce_finish(par)
        at_small[...] = solve(total)
        qv[...] = res - mm(at_small[0:16, :], s_new)
        u = mm(beta_t, zv[...] - omega * vv[...])
        t_new = scatter_finish(par, w_new)
        tv[...] = t_new
        zv[...] = jnp.where(first, t_new, t_new + u)
        drain(ag + ax + ay + az + dd + rs)
        return carry

    lax.fori_loop(0, ITERS, step, 0)

    par = 0
    qq = qv[...]
    yy = wv[...] - mm(at_small[0:16, :], zv[...])
    ax = reduce_x_start(par, sums_of(yy, qq))
    partial = xv[...] + mm(at_small[0:16, :], pv[...])
    ay = reduce_y_start(par)
    az = reduce_z_start(par)
    total = reduce_finish(par)
    out_ref[...] = partial + omega_of(total) * qq
    drain(ax + ay + az)


def per_device(sizes, rhs, diagonal, blocks, block_cols, counts):
    nz, ny = sizes
    vm = pl.BlockSpec(memory_space=pltpu.VMEM)
    sm = pl.BlockSpec(memory_space=pltpu.SMEM)
    vec = pltpu.VMEM((16, 256), F32)
    dma = pltpu.SemaphoreType.DMA
    n_ag = 2 * nz - 1
    out = pl.pallas_call(
        functools.partial(kernel, sizes),
        out_shape=jax.ShapeDtypeStruct((16, 256), F32),
        in_specs=[sm, sm, vm, vm, vm],
        out_specs=vm,
        scratch_shapes=[
            pltpu.VMEM((16, 256, 256), BF16),
            pltpu.VMEM((8 * nz, 16, 128), F32),
            pltpu.VMEM((8 * nz, 16, 128), F32),
            pltpu.VMEM((2 * ny, 2, 16, 128), F32),
            pltpu.VMEM((2, 2 * ny, 2, 16, 128), F32),
            pltpu.VMEM((2, 8, 16, 128), F32),
            pltpu.VMEM((2, ny, 16, 128), F32),
            pltpu.VMEM((2, nz, 16, 128), F32),
            vec, vec, vec, vec, vec, vec, vec, vec, vec, vec,
            pltpu.VMEM((32, 16), F32),
            dma((n_ag,)), dma((2, 2 * nz)),
            dma((2,)), dma((2, 2)),
            dma((2 * ny - 1,)), dma((2, 2 * ny)),
            dma((7,)), dma((2, 8)),
            dma((ny - 1,)), dma((2, ny)),
            dma((nz - 1,)), dma((2, nz)),
        ],
        compiler_params=pltpu.CompilerParams(
            collective_id=0, has_side_effects=True, vmem_limit_bytes=40 * 1024 * 1024
        ),
    )(
        block_cols,
        counts.reshape(-1),
        rhs.T,
        diagonal.reshape(1, -1),
        blocks,
    )
    return out.T


def solution(mesh):
    sizes = (mesh.shape["rows"] // 4, mesh.shape["cols"] // 2)
    in_specs = (
        P(("rows", "cols"), None),
        P(("rows", "cols")),
        P("rows", "cols", None, None),
        P("rows", "cols"),
        P("rows", "cols"),
    )
    return jax.shard_map(
        functools.partial(per_device, sizes),
        mesh=mesh,
        in_specs=in_specs,
        out_specs=P(("rows", "cols"), None),
        check_vma=False,
    )
```

```python
import functools

import jax
import jax.numpy as jnp
from jax import lax
from jax.experimental import pallas as pl
from jax.experimental.pallas import tpu as pltpu
from jax.sharding import PartitionSpec as P

ITERS = 4
MESH = pl.DeviceIdType.MESH
HIGHEST = lax.Precision.HIGHEST
F32 = jnp.float32
BF16 = jnp.bfloat16
NT = (((1,), (1,)), ((), ()))
NN = (((1,), (0,)), ((), ()))


def mm(a, b, dims=NN):
    return lax.dot_general(a, b, dims, precision=HIGHEST, preferred_element_type=F32)


def kernel(
    sizes,
    cols_ref, counts_ref, rhs_hbm, diag_hbm, blocks_hbm, out_ref,
    rhs_ref, diag_ref, blocks_ref, at, gb0, gb1, prod, rsb, arx, ary, arz,
    sh, pv, sv, zv, vv, rv, wv, tv, qv, xv, at_small,
    in_sem, blk_sem, ag_ssem, ag_rsem, fw_rsem, rs_ssem, rs_rsem,
    ax_ssem, ax_rsem, ay_ssem, ay_rsem, az_ssem, az_rsem,
):
    NZ, NY = sizes
    r = lax.axis_index("rows")
    c = lax.axis_index("cols")
    core = lax.rem(r, 2)
    z = lax.rem(lax.div(r, 2), NZ)
    a = lax.div(r, 2 * NZ)
    xh = lax.div(c, NY)
    y = lax.rem(c, NY)
    x = xh * 2 + a
    n_cols = 2 * NY

    rhs_in = pltpu.make_async_copy(rhs_hbm, rhs_ref, in_sem.at[0])
    diag_in = pltpu.make_async_copy(diag_hbm, diag_ref, in_sem.at[1])
    blocks_in = [
        pltpu.make_async_copy(
            blocks_hbm.at[pl.ds(4 * q, 4)], blocks_ref.at[pl.ds(4 * q, 4)], blk_sem.at[q]
        )
        for q in range(4)
    ]
    rhs_in.start()
    diag_in.start()
    for cp in blocks_in:
        cp.start()

    def device(fx, dy, dz, fk):
        xh_ = (1 - xh) if fx & 2 else xh
        a_ = (1 - a) if fx & 1 else a
        k_ = (1 - core) if fk else core
        y_ = lax.rem(y + dy, NY) if dy else y
        z_ = lax.rem(z + dz, NZ) if dz else z
        return ((a_ * NZ + z_) * 2 + k_, xh_ * NY + y_)

    def slot(fk, fa, dz):
        return ((fk * 2 + fa) * NZ + dz) * 2

    def far(n):
        return lambda d: -min(d, n - d)

    z_order = sorted(range(1, NZ), key=far(NZ))
    y_order = sorted(range(NY), key=far(NY))
    far_z = [d for d in z_order if min(d, NZ - d) >= 3]
    mid_z = [d for d in z_order if min(d, NZ - d) < 3]
    scatter_peers = [(2, dy, 0, 0) for dy in y_order] + [(0, dy, 0, 0) for dy in y_order if dy]
    plane_peers = [(fx, 0, 0, fk) for fx in (2, 3, 1, 0) for fk in (1, 0) if (fx, fk) != (0, 0)]
    y_peers = [(0, dy, 0, 1) for dy in y_order if dy]
    z_peers = [(0, 0, dz, 1) for dz in z_order]
    gather_peers = [(0, 0, dz, 1) for dz in z_order] + [(1, 0, dz, 1) for dz in mid_z]
    gather_peers += [(1, 0, 0, 1), (1, 0, 0, 0), (0, 0, 0, 1)]

    barrier = pltpu.get_barrier_semaphore()
    greet = sorted(set(scatter_peers + plane_peers + y_peers + z_peers + gather_peers))
    for peer in greet:
        pl.semaphore_signal(barrier, inc=1, device_id=device(*peer), device_id_type=MESH)

    def prepare():
        for q in range(4):
            blocks_in[q].wait()

            def some(p, carry):
                for b_ in range(2):
                    b = 4 * q + 2 * p + b_
                    cnt = counts_ref[b]
                    for k in range(2):
                        blk = blocks_ref[b, k]
                        blk = jnp.where(k < cnt, blk, 0.0).T
                        hi = blk.astype(BF16)
                        mid = (blk - hi.astype(F32)).astype(BF16)
                        at[b, k * 128:(k + 1) * 128, 0:128] = hi
                        at[b, k * 128:(k + 1) * 128, 128:256] = mid
                return carry

            lax.fori_loop(0, 2, some, 0)

    rhs_in.wait()
    diag_in.wait()
    rhs = rhs_ref[...]
    sh[...] = rhs
    rv[...] = rhs
    wv[...] = rhs
    zv[...] = rhs
    qv[...] = rhs
    xv[...] = -rhs
    zero = jnp.zeros_like(rhs)
    pv[...] = zero
    sv[...] = zero
    vv[...] = zero
    tv[...] = zero
    row16 = lax.broadcasted_iota(jnp.int32, (16, 128), 0)
    lane16 = lax.broadcasted_iota(jnp.int32, (16, 128), 1)
    eye_at_32 = jnp.where(lane16 == row16 + 32, 1.0, 0.0)
    row32 = lax.broadcasted_iota(jnp.int32, (32, 128), 0)
    lane32 = lax.broadcasted_iota(jnp.int32, (32, 128), 1)
    pick = jnp.where(lane32 == row32 + 16, 1.0, 0.0)
    pad96 = jnp.zeros((96, 256), F32)
    pad112 = jnp.zeros((112, 256), F32)
    at_small[...] = jnp.zeros((32, 16), F32)

    pl.semaphore_wait(barrier, len(greet))

    gbs = (gb0, gb1)

    def arrival(ref, sem):
        pltpu.make_async_remote_copy(
            src_ref=ref, dst_ref=ref, send_sem=ag_ssem.at[0], recv_sem=sem,
            device_id=device(0, 0, 0, 1), device_id_type=MESH,
        ).wait_recv()

    def gather_send(par, sends, src, dst, peer, sem):
        cp = pltpu.make_async_remote_copy(
            src_ref=src, dst_ref=dst, send_sem=ag_ssem.at[len(sends)], recv_sem=sem,
            device_id=device(*peer), device_id_type=MESH,
        )
        cp.start()
        sends.append(cp)

    def gather_start(par, vec, sends):
        gb = gbs[par]
        if vec is not None:
            gb[0] = vec[:, 0:128]
            gb[1] = vec[:, 128:256]
        own = gb.at[pl.ds(0, 2)]

        def send(fk, fa, dz):
            s = slot(fk, fa, (NZ - dz) % NZ)
            gather_send(
                par, sends, own, gb.at[pl.ds(s, 2)], (fa, 0, dz, fk), ag_rsem.at[par, s // 2]
            )

        if vec is not None:
            for dz in far_z:
                send(1, 0, dz)
            send(1, 0, 0)
            return
        for dz in mid_z:
            for fa in (1, 0):
                send(1, fa, dz)
        send(1, 1, 0)
        send(0, 1, 0)

    def gather_parts(par, sends, part):
        gb = gbs[par]

        def place(fk, fa, dz, n=1):
            return gb.at[pl.ds(slot(fk, fa, dz), 2 * n)]

        def sem(fk, fa, dz):
            return ag_rsem.at[par, slot(fk, fa, dz) // 2]

        lo, n_far = min(far_z), len(far_z)
        for d in far_z if part == 0 else ():
            dz = NZ - d
            arrival(place(1, 0, dz), sem(1, 0, dz))
            gather_send(par, sends, place(1, 0, dz), place(1, 1, dz), (1, 0, 0, 0), sem(1, 1, dz))
            gather_send(par, sends, place(1, 0, dz), place(0, 1, dz), (1, 0, 0, 1), sem(0, 1, dz))
        if part == 0:
            gather_send(
                par, sends, place(1, 0, lo, n_far), place(0, 0, lo, n_far),
                (0, 0, 0, 1), fw_rsem.at[par]
            )
        for d in mid_z if part == 1 else ():
            dz = NZ - d
            for fa in (0, 1):
                arrival(place(1, fa, dz), sem(1, fa, dz))
                gather_send(
                    par, sends, place(1, fa, dz), place(0, fa, dz), (0, 0, 0, 1), sem(0, fa, dz)
                )
        if part < 2:
            return
        arrival(place(1, 0, 0), sem(1, 0, 0))
        arrival(place(1, 1, 0), sem(1, 1, 0))
        arrival(place(0, 1, 0), sem(0, 1, 0))
        arrival(place(0, 0, lo, n_far), fw_rsem.at[par])
        for d in mid_z:
            dz = NZ - d
            for fa in (0, 1):
                arrival(place(0, fa, dz), sem(0, fa, dz))
        for d in far_z:
            dz = NZ - d
            arrival(place(1, 1, dz), sem(1, 1, dz))
            arrival(place(0, 1, dz), sem(0, 1, dz))

    def block_row(gb, b):
        parts = []
        for k in range(2):
            l = cols_ref[k, b]
            fk = ((l >> 1) & 1) ^ core
            dz = ((l >> 2) + NZ - z) & (NZ - 1)
            fa = (l // (4 * NZ)) ^ a
            parts.append(gb[slot(fk, fa, dz) + (l & 1)])
        v = jnp.concatenate(parts, axis=1)
        vh = v.astype(BF16)
        vm = (v - vh.astype(F32)).astype(BF16)
        both = jnp.concatenate([vh, vm], axis=0)
        full = lax.dot_general(both, at[b], NN, preferred_element_type=F32)
        return full[0:16, 0:128] + (full[16:32, 0:128] + full[0:16, 128:256])

    def products(par):
        gb = gbs[par]
        sends = []
        for n, peer in enumerate(scatter_peers + [(0, 0, 0, 0)]):
            c_ = device(*peer)[1]
            for h in range(2):
                prod[c_, h] = block_row(gb, c_ * 2 + h)
            if n < len(scatter_peers):
                cp = pltpu.make_async_remote_copy(
                    src_ref=prod.at[c_],
                    dst_ref=rsb.at[par, c],
                    send_sem=rs_ssem.at[n],
                    recv_sem=rs_rsem.at[par, c],
                    device_id=device(*peer),
                    device_id_type=MESH,
                )
                cp.start()
                sends.append(cp)
        return sends

    def scatter_finish(par, vec):
        own = prod[c]
        total = jnp.concatenate([own[0], own[1]], axis=1) + diag_ref[...] * vec
        for peer in reversed(scatter_peers):
            c_ = device(*peer)[1]
            pltpu.make_async_remote_copy(
                src_ref=prod.at[c_],
                dst_ref=rsb.at[par, c_],
                send_sem=rs_ssem.at[0],
                recv_sem=rs_rsem.at[par, c_],
                device_id=device(*peer),
                device_id_type=MESH,
            ).wait_recv()
            got = rsb[par, c_]
            total = total + jnp.concatenate([got[0], got[1]], axis=1)
        return total

    def spread(par, part, buf, mine, peers, ssem, rsem):
        buf[par, mine] = part
        sends = []
        for n, peer in enumerate(peers):
            cp = pltpu.make_async_remote_copy(
                src_ref=buf.at[par, mine], dst_ref=buf.at[par, mine],
                send_sem=ssem.at[n], recv_sem=rsem.at[par, mine],
                device_id=device(*peer), device_id_type=MESH,
            )
            cp.start()
            sends.append(cp)
        return sends

    def collect(par, buf, index_of, peers, ssem, rsem):
        for peer in reversed(peers):
            there = index_of(*device(*peer))
            pltpu.make_async_remote_copy(
                src_ref=buf.at[par, there], dst_ref=buf.at[par, there],
                send_sem=ssem.at[0], recv_sem=rsem.at[par, there],
                device_id=device(*peer), device_id_type=MESH,
            ).wait_recv()
        parts = [buf[par, n] for n in range(buf.shape[1])]
        while len(parts) > 1:
            parts = [parts[n] + parts[n + 1] for n in range(0, len(parts), 2)]
        return parts[0]

    def plane_index(r_, c_):
        return (lax.div(c_, NY) * 2 + lax.div(r_, 2 * NZ)) * 2 + lax.rem(r_, 2)

    def y_index(r_, c_):
        return lax.rem(c_, NY)

    def z_index(r_, c_):
        return lax.rem(lax.div(r_, 2), NZ)

    in_plane = (arx, plane_index, plane_peers, ax_ssem, ax_rsem)
    in_y = (ary, y_index, y_peers, ay_ssem, ay_rsem)
    in_z = (arz, z_index, z_peers, az_ssem, az_rsem)

    def reduce_first(par, part):
        buf, index_of, peers, ssem, rsem = in_y
        return spread(par, part, buf, index_of(r, c), peers, ssem, rsem)

    def reduce_second(par):
        part = collect(par, *in_y)
        buf, index_of, peers, ssem, rsem = in_plane
        return spread(par, part, buf, index_of(r, c), peers, ssem, rsem)

    def reduce_third(par):
        part = collect(par, *in_plane)
        buf, index_of, peers, ssem, rsem = in_z
        return spread(par, part, buf, index_of(r, c), peers, ssem, rsem)

    def reduce_finish(par):
        return collect(par, *in_z)

    def drain(sends):
        for cp in sends:
            cp.wait_send()

    def omega_part():
        yy = wv[...] - mm(at_small[0:16, :], zv[...])
        return yy

    def sums_of(yy, qq):
        d = mm(yy, jnp.concatenate([sh[...], pad112], axis=0), NT)
        along = jnp.sum(yy * qq, axis=1, keepdims=True)
        square = jnp.sum(yy * yy, axis=1, keepdims=True)
        return jnp.where(lane16 == 16, along, jnp.where(lane16 == 17, square, d))

    def omega_of(total):
        along = jnp.sum(jnp.where(lane16 == 16, total, 0.0), keepdims=True)
        square = jnp.sum(jnp.where(lane16 == 17, total, 0.0), keepdims=True)
        return along / square

    def solve(total):
        joined = jnp.where(lane16 < 32, total, eye_at_32)
        for i in range(16):
            pivot_row = joined[i:i + 1, :] / joined[i:i + 1, i:i + 1]
            column = joined[:, i:i + 1]
            joined = jnp.where(row16 == i, pivot_row, joined - column * pivot_row)
        return mm(pick, joined, NT)

    def step(i, carry):
        first = i == 0
        par = 0
        ag = []
        gather_start(par, zv[...], ag)
        yy = jnp.where(first, 0.0, wv[...] - mm(at_small[0:16, :], zv[...]))
        qq = qv[...]
        ax = reduce_first(par, sums_of(yy, qq))
        gather_start(par, None, ag)
        pl.when(first)(prepare)
        ay = reduce_second(par)
        gather_parts(par, ag, 0)
        az = reduce_third(par)
        gather_parts(par, ag, 1)
        gather_parts(par, ag, 2)
        rs = products(par)
        total = reduce_finish(par)
        omega = jnp.where(first, 1.0, omega_of(total))
        beta_t = jnp.where(first, 0.0, -mm(total[:, 0:16], at_small[16:32, :]))
        alpha_t = at_small[0:16, :]
        xv[...] = xv[...] + mm(alpha_t, pv[...]) + omega * qq
        res = qq - omega * yy
        new_p = res + mm(beta_t, pv[...] - omega * sv[...])
        kept = mm(beta_t, sv[...] - omega * zv[...])
        left = yy - omega * tv[...]
        vv[...] = scatter_finish(par, zv[...])
        w_new = jnp.where(first, vv[...], left + omega * mm(alpha_t, vv[...]))
        drain(ag + ax + ay + az + rs)
        par = 1
        ag = []
        gather_start(par, w_new, ag)
        s_new = w_new + kept
        d = mm(sh[...], jnp.concatenate([s_new, res, pad96], axis=0), NT)
        ax = reduce_first(par, d)
        gather_start(par, None, ag)
        wv[...] = w_new
        pv[...] = new_p
        sv[...] = s_new
        ay = reduce_second(par)
        gather_parts(par, ag, 0)
        az = reduce_third(par)
        gather_parts(par, ag, 1)
        gather_parts(par, ag, 2)
        rs = products(par)
        total = reduce_finish(par)
        at_small[...] = solve(total)
        qv[...] = res - mm(at_small[0:16, :], s_new)
        u = mm(beta_t, zv[...] - omega * vv[...])
        t_new = scatter_finish(par, w_new)
        tv[...] = t_new
        zv[...] = jnp.where(first, t_new, t_new + u)
        drain(ag + ax + ay + az + rs)
        return carry

    lax.fori_loop(0, ITERS, step, 0)

    par = 0
    qq = qv[...]
    yy = wv[...] - mm(at_small[0:16, :], zv[...])
    ax = reduce_first(par, sums_of(yy, qq))
    partial = xv[...] + mm(at_small[0:16, :], pv[...])
    ay = reduce_second(par)
    az = reduce_third(par)
    total = reduce_finish(par)
    out_ref[...] = partial + omega_of(total) * qq
    drain(ax + ay + az)


def per_device(sizes, rhs, diagonal, blocks, block_cols, counts):
    nz, ny = sizes
    vm = pl.BlockSpec(memory_space=pltpu.VMEM)
    hbm = pl.BlockSpec(memory_space=pl.ANY)
    sm = pl.BlockSpec(memory_space=pltpu.SMEM)
    vec = pltpu.VMEM((16, 256), F32)
    dma = pltpu.SemaphoreType.DMA
    out = pl.pallas_call(
        functools.partial(kernel, sizes),
        out_shape=jax.ShapeDtypeStruct((16, 256), F32),
        in_specs=[sm, sm, hbm, hbm, hbm],
        out_specs=vm,
        scratch_shapes=[
            vec,
            pltpu.VMEM((1, 256), F32),
            pltpu.VMEM((16, 2, 128, 128), F32),
            pltpu.VMEM((16, 256, 256), BF16),
            pltpu.VMEM((8 * nz, 16, 128), F32),
            pltpu.VMEM((8 * nz, 16, 128), F32),
            pltpu.VMEM((2 * ny, 2, 16, 128), F32),
            pltpu.VMEM((2, 2 * ny, 2, 16, 128), F32),
            pltpu.VMEM((2, 8, 16, 128), F32),
            pltpu.VMEM((2, ny, 16, 128), F32),
            pltpu.VMEM((2, nz, 16, 128), F32),
            vec, vec, vec, vec, vec, vec, vec, vec, vec, vec,
            pltpu.VMEM((32, 16), F32),
            dma((2,)), dma((4,)),
            dma((40,)), dma((2, 4 * nz)), dma((2,)),
            dma((2 * ny - 1,)), dma((2, 2 * ny)),
            dma((7,)), dma((2, 8)),
            dma((ny - 1,)), dma((2, ny)),
            dma((nz - 1,)), dma((2, nz)),
        ],
        compiler_params=pltpu.CompilerParams(
            collective_id=0, has_side_effects=True, vmem_limit_bytes=60 * 1024 * 1024
        ),
    )(
        block_cols.T,
        counts.reshape(-1),
        rhs.T,
        diagonal.reshape(1, -1),
        blocks,
    )
    return out.T


def solution(mesh):
    sizes = (mesh.shape["rows"] // 4, mesh.shape["cols"] // 2)
    in_specs = (
        P(("rows", "cols"), None),
        P(("rows", "cols")),
        P("rows", "cols", None, None),
        P("rows", "cols"),
        P("rows", "cols"),
    )
    return jax.shard_map(
        functools.partial(per_device, sizes),
        mesh=mesh,
        in_specs=in_specs,
        out_specs=P(("rows", "cols"), None),
        check_vma=False,
    )
```

```python
import functools

import jax
import jax.numpy as jnp
from jax import lax
from jax.experimental import pallas as pl
from jax.experimental.pallas import tpu as pltpu
from jax.sharding import PartitionSpec as P

ITERS = 4
MESH = pl.DeviceIdType.MESH
HIGHEST = lax.Precision.HIGHEST
F32 = jnp.float32
BF16 = jnp.bfloat16
NT = (((1,), (1,)), ((), ()))
NN = (((1,), (0,)), ((), ()))


def mm(a, b, dims=NN):
    return lax.dot_general(a, b, dims, precision=HIGHEST, preferred_element_type=F32)


def kernel(
    sizes,
    cols_ref, counts_ref, rhs_hbm, diag_hbm, blocks_hbm, out_ref,
    rhs_ref, diag_ref, blocks_ref, at, gb0, gb1, prod, rsb, arx, ary, arz,
    sh, pv, sv, zv, vv, rv, wv, tv, qv, xv, at_small,
    in_sem, blk_sem, ag_ssem, ag_rsem, fw_rsem, rs_ssem, rs_rsem,
    ax_ssem, ax_rsem, ay_ssem, ay_rsem, az_ssem, az_rsem,
):
    NZ, NY = sizes
    r = lax.axis_index("rows")
    c = lax.axis_index("cols")
    core = lax.rem(r, 2)
    z = lax.rem(lax.div(r, 2), NZ)
    a = lax.div(r, 2 * NZ)
    xh = lax.div(c, NY)
    y = lax.rem(c, NY)
    x = xh * 2 + a
    n_cols = 2 * NY

    rhs_in = pltpu.make_async_copy(rhs_hbm, rhs_ref, in_sem.at[0])
    diag_in = pltpu.make_async_copy(diag_hbm, diag_ref, in_sem.at[1])
    blocks_in = [
        pltpu.make_async_copy(
            blocks_hbm.at[pl.ds(4 * q, 4)], blocks_ref.at[pl.ds(4 * q, 4)], blk_sem.at[q]
        )
        for q in range(4)
    ]
    rhs_in.start()
    diag_in.start()
    for cp in blocks_in:
        cp.start()

    def device(fx, dy, dz, fk):
        xh_ = (1 - xh) if fx & 2 else xh
        a_ = (1 - a) if fx & 1 else a
        k_ = (1 - core) if fk else core
        y_ = lax.rem(y + dy, NY) if dy else y
        z_ = lax.rem(z + dz, NZ) if dz else z
        return ((a_ * NZ + z_) * 2 + k_, xh_ * NY + y_)

    def slot(fk, fa, dz):
        return ((fk * 2 + fa) * NZ + dz) * 2

    def far(n):
        return lambda d: -min(d, n - d)

    z_order = sorted(range(1, NZ), key=far(NZ))
    y_order = sorted(range(NY), key=far(NY))
    far_z = [d for d in z_order if min(d, NZ - d) >= 3]
    mid_z = [d for d in z_order if min(d, NZ - d) < 3]
    scatter_peers = [(2, dy, 0, 0) for dy in y_order] + [(0, dy, 0, 0) for dy in y_order if dy]
    plane_peers = [(fx, 0, 0, fk) for fx in (2, 3, 1, 0) for fk in (1, 0) if (fx, fk) != (0, 0)]
    y_peers = [(0, dy, 0, 1) for dy in y_order if dy]
    z_peers = [(0, 0, dz, 1) for dz in z_order]
    gather_peers = [(0, 0, dz, 1) for dz in z_order] + [(1, 0, dz, 1) for dz in mid_z]
    gather_peers += [(1, 0, 0, 1), (1, 0, 0, 0), (0, 0, 0, 1)]

    barrier = pltpu.get_barrier_semaphore()
    greet = sorted(set(scatter_peers + plane_peers + y_peers + z_peers + gather_peers))
    for peer in greet:
        pl.semaphore_signal(barrier, inc=1, device_id=device(*peer), device_id_type=MESH)

    def prepare():
        for q in range(4):
            blocks_in[q].wait()

            def some(p, carry):
                for b_ in range(2):
                    b = 4 * q + 2 * p + b_
                    cnt = counts_ref[b]
                    for k in range(2):
                        blk = blocks_ref[b, k]
                        blk = jnp.where(k < cnt, blk, 0.0).T
                        hi = blk.astype(BF16)
                        mid = (blk - hi.astype(F32)).astype(BF16)
                        at[b, k * 128:(k + 1) * 128, 0:128] = hi
                        at[b, k * 128:(k + 1) * 128, 128:256] = mid
                return carry

            lax.fori_loop(0, 2, some, 0)

    rhs_in.wait()
    diag_in.wait()
    rhs = rhs_ref[...]
    sh[...] = rhs
    rv[...] = rhs
    wv[...] = rhs
    zv[...] = rhs
    qv[...] = rhs
    xv[...] = -rhs
    zero = jnp.zeros_like(rhs)
    pv[...] = zero
    sv[...] = zero
    vv[...] = zero
    tv[...] = zero
    row16 = lax.broadcasted_iota(jnp.int32, (16, 128), 0)
    lane16 = lax.broadcasted_iota(jnp.int32, (16, 128), 1)
    eye_at_32 = jnp.where(lane16 == row16 + 32, 1.0, 0.0)
    row32 = lax.broadcasted_iota(jnp.int32, (32, 128), 0)
    lane32 = lax.broadcasted_iota(jnp.int32, (32, 128), 1)
    pick = jnp.where(lane32 == row32 + 16, 1.0, 0.0)
    pad96 = jnp.zeros((96, 256), F32)
    pad112 = jnp.zeros((112, 256), F32)
    at_small[...] = jnp.zeros((32, 16), F32)

    prepare()
    pl.semaphore_wait(barrier, len(greet))

    gbs = (gb0, gb1)

    def arrival(ref, sem):
        pltpu.make_async_remote_copy(
            src_ref=ref, dst_ref=ref, send_sem=ag_ssem.at[0], recv_sem=sem,
            device_id=device(0, 0, 0, 1), device_id_type=MESH,
        ).wait_recv()

    def gather_send(par, sends, src, dst, peer, sem):
        cp = pltpu.make_async_remote_copy(
            src_ref=src, dst_ref=dst, send_sem=ag_ssem.at[len(sends)], recv_sem=sem,
            device_id=device(*peer), device_id_type=MESH,
        )
        cp.start()
        sends.append(cp)

    def gather_start(par, vec, sends):
        gb = gbs[par]
        if vec is not None:
            gb[0] = vec[:, 0:128]
            gb[1] = vec[:, 128:256]
        own = gb.at[pl.ds(0, 2)]

        def send(fk, fa, dz):
            s = slot(fk, fa, (NZ - dz) % NZ)
            gather_send(
                par, sends, own, gb.at[pl.ds(s, 2)], (fa, 0, dz, fk), ag_rsem.at[par, s // 2]
            )

        if vec is not None:
            for dz in far_z:
                send(1, 0, dz)
            send(1, 0, 0)
            return
        for dz in mid_z:
            for fa in (1, 0):
                send(1, fa, dz)
        send(1, 1, 0)
        send(0, 1, 0)

    def gather_parts(par, sends, part):
        gb = gbs[par]

        def place(fk, fa, dz, n=1):
            return gb.at[pl.ds(slot(fk, fa, dz), 2 * n)]

        def sem(fk, fa, dz):
            return ag_rsem.at[par, slot(fk, fa, dz) // 2]

        lo, n_far = min(far_z), len(far_z)
        for d in far_z if part == 0 else ():
            dz = NZ - d
            arrival(place(1, 0, dz), sem(1, 0, dz))
            gather_send(par, sends, place(1, 0, dz), place(1, 1, dz), (1, 0, 0, 0), sem(1, 1, dz))
            gather_send(par, sends, place(1, 0, dz), place(0, 1, dz), (1, 0, 0, 1), sem(0, 1, dz))
        if part == 0:
            gather_send(
                par, sends, place(1, 0, lo, n_far), place(0, 0, lo, n_far),
                (0, 0, 0, 1), fw_rsem.at[par]
            )
        for d in mid_z if part == 1 else ():
            dz = NZ - d
            for fa in (0, 1):
                arrival(place(1, fa, dz), sem(1, fa, dz))
                gather_send(
                    par, sends, place(1, fa, dz), place(0, fa, dz), (0, 0, 0, 1), sem(0, fa, dz)
                )
        if part < 2:
            return
        arrival(place(1, 0, 0), sem(1, 0, 0))
        arrival(place(1, 1, 0), sem(1, 1, 0))
        arrival(place(0, 1, 0), sem(0, 1, 0))
        arrival(place(0, 0, lo, n_far), fw_rsem.at[par])
        for d in mid_z:
            dz = NZ - d
            for fa in (0, 1):
                arrival(place(0, fa, dz), sem(0, fa, dz))
        for d in far_z:
            dz = NZ - d
            arrival(place(1, 1, dz), sem(1, 1, dz))
            arrival(place(0, 1, dz), sem(0, 1, dz))

    def block_row(gb, b):
        parts = []
        for k in range(2):
            l = cols_ref[k, b]
            fk = ((l >> 1) & 1) ^ core
            dz = ((l >> 2) + NZ - z) & (NZ - 1)
            fa = (l // (4 * NZ)) ^ a
            parts.append(gb[slot(fk, fa, dz) + (l & 1)])
        v = jnp.concatenate(parts, axis=1)
        vh = v.astype(BF16)
        vm = (v - vh.astype(F32)).astype(BF16)
        both = jnp.concatenate([vh, vm], axis=0)
        full = lax.dot_general(both, at[b], NN, preferred_element_type=F32)
        return full[0:16, 0:128] + (full[16:32, 0:128] + full[0:16, 128:256])

    def products(par):
        gb = gbs[par]
        sends = []
        for n, peer in enumerate(scatter_peers + [(0, 0, 0, 0)]):
            c_ = device(*peer)[1]
            for h in range(2):
                prod[c_, h] = block_row(gb, c_ * 2 + h)
            if n < len(scatter_peers):
                cp = pltpu.make_async_remote_copy(
                    src_ref=prod.at[c_],
                    dst_ref=rsb.at[par, c],
                    send_sem=rs_ssem.at[n],
                    recv_sem=rs_rsem.at[par, c],
                    device_id=device(*peer),
                    device_id_type=MESH,
                )
                cp.start()
                sends.append(cp)
        return sends

    def scatter_finish(par, vec):
        own = prod[c]
        total = jnp.concatenate([own[0], own[1]], axis=1) + diag_ref[...] * vec
        for peer in reversed(scatter_peers):
            c_ = device(*peer)[1]
            pltpu.make_async_remote_copy(
                src_ref=prod.at[c_],
                dst_ref=rsb.at[par, c_],
                send_sem=rs_ssem.at[0],
                recv_sem=rs_rsem.at[par, c_],
                device_id=device(*peer),
                device_id_type=MESH,
            ).wait_recv()
            got = rsb[par, c_]
            total = total + jnp.concatenate([got[0], got[1]], axis=1)
        return total

    def spread(par, part, buf, mine, peers, ssem, rsem):
        buf[par, mine] = part
        sends = []
        for n, peer in enumerate(peers):
            cp = pltpu.make_async_remote_copy(
                src_ref=buf.at[par, mine], dst_ref=buf.at[par, mine],
                send_sem=ssem.at[n], recv_sem=rsem.at[par, mine],
                device_id=device(*peer), device_id_type=MESH,
            )
            cp.start()
            sends.append(cp)
        return sends

    def collect(par, buf, index_of, peers, ssem, rsem):
        for peer in reversed(peers):
            there = index_of(*device(*peer))
            pltpu.make_async_remote_copy(
                src_ref=buf.at[par, there], dst_ref=buf.at[par, there],
                send_sem=ssem.at[0], recv_sem=rsem.at[par, there],
                device_id=device(*peer), device_id_type=MESH,
            ).wait_recv()
        parts = [buf[par, n] for n in range(buf.shape[1])]
        while len(parts) > 1:
            parts = [parts[n] + parts[n + 1] for n in range(0, len(parts), 2)]
        return parts[0]

    def plane_index(r_, c_):
        return (lax.div(c_, NY) * 2 + lax.div(r_, 2 * NZ)) * 2 + lax.rem(r_, 2)

    def y_index(r_, c_):
        return lax.rem(c_, NY)

    def z_index(r_, c_):
        return lax.rem(lax.div(r_, 2), NZ)

    in_plane = (arx, plane_index, plane_peers, ax_ssem, ax_rsem)
    in_y = (ary, y_index, y_peers, ay_ssem, ay_rsem)
    in_z = (arz, z_index, z_peers, az_ssem, az_rsem)

    def reduce_first(par, part):
        buf, index_of, peers, ssem, rsem = in_y
        return spread(par, part, buf, index_of(r, c), peers, ssem, rsem)

    def reduce_second(par):
        part = collect(par, *in_y)
        buf, index_of, peers, ssem, rsem = in_plane
        return spread(par, part, buf, index_of(r, c), peers, ssem, rsem)

    def reduce_third(par):
        part = collect(par, *in_plane)
        buf, index_of, peers, ssem, rsem = in_z
        return spread(par, part, buf, index_of(r, c), peers, ssem, rsem)

    def reduce_finish(par):
        return collect(par, *in_z)

    def drain(sends):
        for cp in sends:
            cp.wait_send()

    def omega_part():
        yy = wv[...] - mm(at_small[0:16, :], zv[...])
        return yy

    def sums_of(yy, qq):
        d = mm(yy, jnp.concatenate([sh[...], pad112], axis=0), NT)
        along = jnp.sum(yy * qq, axis=1, keepdims=True)
        square = jnp.sum(yy * yy, axis=1, keepdims=True)
        return jnp.where(lane16 == 16, along, jnp.where(lane16 == 17, square, d))

    def omega_of(total):
        along = jnp.sum(jnp.where(lane16 == 16, total, 0.0), keepdims=True)
        square = jnp.sum(jnp.where(lane16 == 17, total, 0.0), keepdims=True)
        return along / square

    def solve(total):
        joined = jnp.where(lane16 < 32, total, eye_at_32)
        for i in range(16):
            pivot_row = joined[i:i + 1, :] / joined[i:i + 1, i:i + 1]
            column = joined[:, i:i + 1]
            joined = jnp.where(row16 == i, pivot_row, joined - column * pivot_row)
        return mm(pick, joined, NT)

    def step(i, carry):
        first = i == 0
        par = 0
        ag = []
        gather_start(par, zv[...], ag)
        yy = jnp.where(first, 0.0, wv[...] - mm(at_small[0:16, :], zv[...]))
        qq = qv[...]
        ax = reduce_first(par, sums_of(yy, qq))
        gather_start(par, None, ag)
        ay = reduce_second(par)
        gather_parts(par, ag, 0)
        az = reduce_third(par)
        gather_parts(par, ag, 1)
        gather_parts(par, ag, 2)
        rs = products(par)
        total = reduce_finish(par)
        omega = jnp.where(first, 1.0, omega_of(total))
        beta_t = jnp.where(first, 0.0, -mm(total[:, 0:16], at_small[16:32, :]))
        alpha_t = at_small[0:16, :]
        xv[...] = xv[...] + mm(alpha_t, pv[...]) + omega * qq
        res = qq - omega * yy
        new_p = res + mm(beta_t, pv[...] - omega * sv[...])
        kept = mm(beta_t, sv[...] - omega * zv[...])
        left = yy - omega * tv[...]
        drain(ag + ax + ay + az + rs)
        vv[...] = scatter_finish(par, zv[...])
        w_new = jnp.where(first, vv[...], left + omega * mm(alpha_t, vv[...]))
        par = 1
        ag = []
        gather_start(par, w_new, ag)
        s_new = w_new + kept
        d = mm(sh[...], jnp.concatenate([s_new, res, pad96], axis=0), NT)
        ax = reduce_first(par, d)
        gather_start(par, None, ag)
        wv[...] = w_new
        pv[...] = new_p
        sv[...] = s_new
        ay = reduce_second(par)
        gather_parts(par, ag, 0)
        az = reduce_third(par)
        gather_parts(par, ag, 1)
        gather_parts(par, ag, 2)
        rs = products(par)
        total = reduce_finish(par)
        at_small[...] = solve(total)
        qv[...] = res - mm(at_small[0:16, :], s_new)
        u = mm(beta_t, zv[...] - omega * vv[...])
        drain(ag + ax + ay + az + rs)
        t_new = scatter_finish(par, w_new)
        tv[...] = t_new
        zv[...] = jnp.where(first, t_new, t_new + u)
        return carry

    lax.fori_loop(0, ITERS, step, 0)

    par = 0
    qq = qv[...]
    yy = wv[...] - mm(at_small[0:16, :], zv[...])
    ax = reduce_first(par, sums_of(yy, qq))
    partial = xv[...] + mm(at_small[0:16, :], pv[...])
    ay = reduce_second(par)
    az = reduce_third(par)
    total = reduce_finish(par)
    out_ref[...] = partial + omega_of(total) * qq
    drain(ax + ay + az)


def per_device(sizes, rhs, diagonal, blocks, block_cols, counts):
    nz, ny = sizes
    vm = pl.BlockSpec(memory_space=pltpu.VMEM)
    hbm = pl.BlockSpec(memory_space=pl.ANY)
    sm = pl.BlockSpec(memory_space=pltpu.SMEM)
    vec = pltpu.VMEM((16, 256), F32)
    dma = pltpu.SemaphoreType.DMA
    out = pl.pallas_call(
        functools.partial(kernel, sizes),
        out_shape=jax.ShapeDtypeStruct((16, 256), F32),
        in_specs=[sm, sm, hbm, hbm, hbm],
        out_specs=vm,
        scratch_shapes=[
            vec,
            pltpu.VMEM((1, 256), F32),
            pltpu.VMEM((16, 2, 128, 128), F32),
            pltpu.VMEM((16, 256, 256), BF16),
            pltpu.VMEM((8 * nz, 16, 128), F32),
            pltpu.VMEM((8 * nz, 16, 128), F32),
            pltpu.VMEM((2 * ny, 2, 16, 128), F32),
            pltpu.VMEM((2, 2 * ny, 2, 16, 128), F32),
            pltpu.VMEM((2, 8, 16, 128), F32),
            pltpu.VMEM((2, ny, 16, 128), F32),
            pltpu.VMEM((2, nz, 16, 128), F32),
            vec, vec, vec, vec, vec, vec, vec, vec, vec, vec,
            pltpu.VMEM((32, 16), F32),
            dma((2,)), dma((4,)),
            dma((40,)), dma((2, 4 * nz)), dma((2,)),
            dma((2 * ny - 1,)), dma((2, 2 * ny)),
            dma((7,)), dma((2, 8)),
            dma((ny - 1,)), dma((2, ny)),
            dma((nz - 1,)), dma((2, nz)),
        ],
        compiler_params=pltpu.CompilerParams(
            collective_id=0, has_side_effects=True, vmem_limit_bytes=60 * 1024 * 1024
        ),
    )(
        block_cols.T,
        counts.reshape(-1),
        rhs.T,
        diagonal.reshape(1, -1),
        blocks,
    )
    return out.T


def solution(mesh):
    sizes = (mesh.shape["rows"] // 4, mesh.shape["cols"] // 2)
    in_specs = (
        P(("rows", "cols"), None),
        P(("rows", "cols")),
        P("rows", "cols", None, None),
        P("rows", "cols"),
        P("rows", "cols"),
    )
    return jax.shard_map(
        functools.partial(per_device, sizes),
        mesh=mesh,
        in_specs=in_specs,
        out_specs=P(("rows", "cols"), None),
        check_vma=False,
    )
```

```python
import functools

import jax
import jax.numpy as jnp
from jax import lax
from jax.experimental import pallas as pl
from jax.experimental.pallas import tpu as pltpu
from jax.sharding import PartitionSpec as P

ITERS = 4
MESH = pl.DeviceIdType.MESH
HIGHEST = lax.Precision.HIGHEST
F32 = jnp.float32
BF16 = jnp.bfloat16
NT = (((1,), (1,)), ((), ()))
NN = (((1,), (0,)), ((), ()))


def mm(a, b, dims=NN):
    return lax.dot_general(a, b, dims, precision=HIGHEST, preferred_element_type=F32)


def kernel(
    sizes,
    cols_ref, counts_ref, rhs_hbm, diag_hbm, blocks_hbm, out_ref,
    rhs_ref, diag_ref, blocks_ref, at, gb0, gb1, prod, rsb, arx, ary, arz,
    sh, pv, sv, zv, vv, rv, wv, tv, qv, xv, at_small,
    in_sem, blk_sem, ag_ssem, ag_rsem, fw_rsem, rs_ssem, rs_rsem,
    ax_ssem, ax_rsem, ay_ssem, ay_rsem, az_ssem, az_rsem,
):
    NZ, NY = sizes
    r = lax.axis_index("rows")
    c = lax.axis_index("cols")
    core = lax.rem(r, 2)
    z = lax.rem(lax.div(r, 2), NZ)
    a = lax.div(r, 2 * NZ)
    xh = lax.div(c, NY)
    y = lax.rem(c, NY)
    x = xh * 2 + a
    n_cols = 2 * NY

    rhs_in = pltpu.make_async_copy(rhs_hbm, rhs_ref, in_sem.at[0])
    diag_in = pltpu.make_async_copy(diag_hbm, diag_ref, in_sem.at[1])
    blocks_in = [
        pltpu.make_async_copy(
            blocks_hbm.at[pl.ds(4 * q, 4)], blocks_ref.at[pl.ds(4 * q, 4)], blk_sem.at[q]
        )
        for q in range(4)
    ]
    rhs_in.start()
    diag_in.start()
    for cp in blocks_in:
        cp.start()

    def device(fx, dy, dz, fk):
        xh_ = (1 - xh) if fx & 2 else xh
        a_ = (1 - a) if fx & 1 else a
        k_ = (1 - core) if fk else core
        y_ = lax.rem(y + dy, NY) if dy else y
        z_ = lax.rem(z + dz, NZ) if dz else z
        return ((a_ * NZ + z_) * 2 + k_, xh_ * NY + y_)

    def slot(fk, fa, dz):
        return ((fk * 2 + fa) * NZ + dz) * 2

    def far(n):
        return lambda d: -min(d, n - d)

    z_order = sorted(range(1, NZ), key=far(NZ))
    y_order = sorted(range(NY), key=far(NY))
    far_z = [d for d in z_order if min(d, NZ - d) >= 4]
    mid_z = [d for d in z_order if min(d, NZ - d) < 4]
    scatter_peers = [(2, dy, 0, 0) for dy in y_order] + [(0, dy, 0, 0) for dy in y_order if dy]
    chip_peers = [(0, 0, 0, 1)]
    plane_peers = [(fx, dy, 0, 1) for fx in (2, 3, 1, 0) for dy in y_order if (fx, dy) != (0, 0)]
    z_peers = [(0, 0, dz, 1) for dz in z_order]
    gather_peers = [(0, 0, dz, 1) for dz in z_order] + [(1, 0, dz, 1) for dz in mid_z]
    gather_peers += [(1, 0, 0, 1), (1, 0, 0, 0), (0, 0, 0, 1)]

    barrier = pltpu.get_barrier_semaphore()
    greet = sorted(set(scatter_peers + plane_peers + z_peers + gather_peers))
    for peer in greet:
        pl.semaphore_signal(barrier, inc=1, device_id=device(*peer), device_id_type=MESH)

    def prepare():
        for q in range(4):
            blocks_in[q].wait()

            def some(p, carry):
                for b_ in range(2):
                    b = 4 * q + 2 * p + b_
                    cnt = counts_ref[b]
                    for k in range(2):
                        blk = blocks_ref[b, k]
                        blk = jnp.where(k < cnt, blk, 0.0).T
                        hi = blk.astype(BF16)
                        mid = (blk - hi.astype(F32)).astype(BF16)
                        at[b, k * 128:(k + 1) * 128, 0:128] = hi
                        at[b, k * 128:(k + 1) * 128, 128:256] = mid
                return carry

            lax.fori_loop(0, 2, some, 0)

    rhs_in.wait()
    diag_in.wait()
    rhs = rhs_ref[...]
    sh[...] = rhs
    rv[...] = rhs
    wv[...] = rhs
    zv[...] = rhs
    qv[...] = rhs
    xv[...] = -rhs
    zero = jnp.zeros_like(rhs)
    pv[...] = zero
    sv[...] = zero
    vv[...] = zero
    tv[...] = zero
    row16 = lax.broadcasted_iota(jnp.int32, (16, 128), 0)
    lane16 = lax.broadcasted_iota(jnp.int32, (16, 128), 1)
    eye_at_32 = jnp.where(lane16 == row16 + 32, 1.0, 0.0)
    row32 = lax.broadcasted_iota(jnp.int32, (32, 128), 0)
    lane32 = lax.broadcasted_iota(jnp.int32, (32, 128), 1)
    pick = jnp.where(lane32 == row32 + 16, 1.0, 0.0)
    pad96 = jnp.zeros((96, 256), F32)
    pad112 = jnp.zeros((112, 256), F32)
    at_small[...] = jnp.zeros((32, 16), F32)

    prepare()
    pl.semaphore_wait(barrier, len(greet))

    gbs = (gb0, gb1)

    def arrival(ref, sem):
        pltpu.make_async_remote_copy(
            src_ref=ref, dst_ref=ref, send_sem=ag_ssem.at[0], recv_sem=sem,
            device_id=device(0, 0, 0, 1), device_id_type=MESH,
        ).wait_recv()

    def gather_send(par, sends, src, dst, peer, sem):
        cp = pltpu.make_async_remote_copy(
            src_ref=src, dst_ref=dst, send_sem=ag_ssem.at[len(sends)], recv_sem=sem,
            device_id=device(*peer), device_id_type=MESH,
        )
        cp.start()
        sends.append(cp)

    def gather_start(par, vec, sends):
        gb = gbs[par]
        if vec is not None:
            gb[0] = vec[:, 0:128]
            gb[1] = vec[:, 128:256]
        own = gb.at[pl.ds(0, 2)]

        def send(fk, fa, dz):
            s = slot(fk, fa, (NZ - dz) % NZ)
            gather_send(
                par, sends, own, gb.at[pl.ds(s, 2)], (fa, 0, dz, fk), ag_rsem.at[par, s // 2]
            )

        if vec is not None:
            for dz in far_z:
                send(1, 0, dz)
            for dz in mid_z[:2]:
                for fa in (1, 0):
                    send(1, fa, dz)
            send(1, 0, 0)
            return
        for dz in mid_z[2:]:
            for fa in (1, 0):
                send(1, fa, dz)
        send(1, 1, 0)
        send(0, 1, 0)

    def gather_parts(par, sends, part):
        gb = gbs[par]

        def place(fk, fa, dz, n=1):
            return gb.at[pl.ds(slot(fk, fa, dz), 2 * n)]

        def sem(fk, fa, dz):
            return ag_rsem.at[par, slot(fk, fa, dz) // 2]

        lo, n_far = min(far_z), len(far_z)
        for d in far_z if part == 0 else ():
            dz = NZ - d
            arrival(place(1, 0, dz), sem(1, 0, dz))
            gather_send(par, sends, place(1, 0, dz), place(1, 1, dz), (1, 0, 0, 0), sem(1, 1, dz))
            gather_send(par, sends, place(1, 0, dz), place(0, 1, dz), (1, 0, 0, 1), sem(0, 1, dz))
        if part == 0:
            gather_send(
                par, sends, place(1, 0, lo, n_far), place(0, 0, lo, n_far),
                (0, 0, 0, 1), fw_rsem.at[par]
            )
        for d in mid_z if part == 1 else ():
            dz = NZ - d
            for fa in (0, 1):
                arrival(place(1, fa, dz), sem(1, fa, dz))
                gather_send(
                    par, sends, place(1, fa, dz), place(0, fa, dz), (0, 0, 0, 1), sem(0, fa, dz)
                )
        if part < 2:
            return
        arrival(place(1, 0, 0), sem(1, 0, 0))
        arrival(place(1, 1, 0), sem(1, 1, 0))
        arrival(place(0, 1, 0), sem(0, 1, 0))
        arrival(place(0, 0, lo, n_far), fw_rsem.at[par])
        for d in mid_z:
            dz = NZ - d
            for fa in (0, 1):
                arrival(place(0, fa, dz), sem(0, fa, dz))
        for d in far_z:
            dz = NZ - d
            arrival(place(1, 1, dz), sem(1, 1, dz))
            arrival(place(0, 1, dz), sem(0, 1, dz))

    def block_row(gb, b):
        parts = []
        for k in range(2):
            l = cols_ref[k, b]
            fk = ((l >> 1) & 1) ^ core
            dz = ((l >> 2) + NZ - z) & (NZ - 1)
            fa = (l // (4 * NZ)) ^ a
            parts.append(gb[slot(fk, fa, dz) + (l & 1)])
        v = jnp.concatenate(parts, axis=1)
        vh = v.astype(BF16)
        vm = (v - vh.astype(F32)).astype(BF16)
        both = jnp.concatenate([vh, vm], axis=0)
        full = lax.dot_general(both, at[b], NN, preferred_element_type=F32)
        return full[0:16, 0:128] + (full[16:32, 0:128] + full[0:16, 128:256])

    def products(par):
        gb = gbs[par]
        sends = []
        for n, peer in enumerate(scatter_peers + [(0, 0, 0, 0)]):
            c_ = device(*peer)[1]
            for h in range(2):
                prod[c_, h] = block_row(gb, c_ * 2 + h)
            if n < len(scatter_peers):
                cp = pltpu.make_async_remote_copy(
                    src_ref=prod.at[c_],
                    dst_ref=rsb.at[par, c],
                    send_sem=rs_ssem.at[n],
                    recv_sem=rs_rsem.at[par, c],
                    device_id=device(*peer),
                    device_id_type=MESH,
                )
                cp.start()
                sends.append(cp)
        return sends

    def scatter_finish(par, vec):
        own = prod[c]
        total = jnp.concatenate([own[0], own[1]], axis=1) + diag_ref[...] * vec
        for peer in reversed(scatter_peers):
            c_ = device(*peer)[1]
            pltpu.make_async_remote_copy(
                src_ref=prod.at[c_],
                dst_ref=rsb.at[par, c_],
                send_sem=rs_ssem.at[0],
                recv_sem=rs_rsem.at[par, c_],
                device_id=device(*peer),
                device_id_type=MESH,
            ).wait_recv()
            got = rsb[par, c_]
            total = total + jnp.concatenate([got[0], got[1]], axis=1)
        return total

    def spread(par, part, buf, mine, peers, ssem, rsem):
        buf[par, mine] = part
        sends = []
        for n, peer in enumerate(peers):
            cp = pltpu.make_async_remote_copy(
                src_ref=buf.at[par, mine], dst_ref=buf.at[par, mine],
                send_sem=ssem.at[n], recv_sem=rsem.at[par, mine],
                device_id=device(*peer), device_id_type=MESH,
            )
            cp.start()
            sends.append(cp)
        return sends

    def collect(par, buf, index_of, peers, ssem, rsem):
        for peer in reversed(peers):
            there = index_of(*device(*peer))
            pltpu.make_async_remote_copy(
                src_ref=buf.at[par, there], dst_ref=buf.at[par, there],
                send_sem=ssem.at[0], recv_sem=rsem.at[par, there],
                device_id=device(*peer), device_id_type=MESH,
            ).wait_recv()
        parts = [buf[par, n] for n in range(buf.shape[1])]
        while len(parts) > 1:
            parts = [parts[n] + parts[n + 1] for n in range(0, len(parts), 2)]
        return parts[0]

    def chip_index(r_, c_):
        return lax.rem(r_, 2)

    def plane_index(r_, c_):
        return (lax.div(c_, NY) * 2 + lax.div(r_, 2 * NZ)) * NY + lax.rem(c_, NY)

    def z_index(r_, c_):
        return lax.rem(lax.div(r_, 2), NZ)

    in_plane = (arx, plane_index, plane_peers, ax_ssem, ax_rsem)
    in_chip = (ary, chip_index, chip_peers, ay_ssem, ay_rsem)
    in_z = (arz, z_index, z_peers, az_ssem, az_rsem)

    def reduce_first(par, part):
        buf, index_of, peers, ssem, rsem = in_chip
        return spread(par, part, buf, index_of(r, c), peers, ssem, rsem)

    def reduce_second(par):
        part = collect(par, *in_chip)
        buf, index_of, peers, ssem, rsem = in_plane
        return spread(par, part, buf, index_of(r, c), peers, ssem, rsem)

    def reduce_third(par):
        part = collect(par, *in_plane)
        buf, index_of, peers, ssem, rsem = in_z
        return spread(par, part, buf, index_of(r, c), peers, ssem, rsem)

    def reduce_finish(par):
        return collect(par, *in_z)

    def drain(sends):
        for cp in sends:
            cp.wait_send()

    def omega_part():
        yy = wv[...] - mm(at_small[0:16, :], zv[...])
        return yy

    def sums_of(yy, qq):
        d = mm(yy, jnp.concatenate([sh[...], pad112], axis=0), NT)
        along = jnp.sum(yy * qq, axis=1, keepdims=True)
        square = jnp.sum(yy * yy, axis=1, keepdims=True)
        return jnp.where(lane16 == 16, along, jnp.where(lane16 == 17, square, d))

    def omega_of(total):
        along = jnp.sum(jnp.where(lane16 == 16, total, 0.0), keepdims=True)
        square = jnp.sum(jnp.where(lane16 == 17, total, 0.0), keepdims=True)
        return along / square

    def solve(total):
        joined = jnp.where(lane16 < 32, total, eye_at_32)
        for i in range(16):
            pivot_row = joined[i:i + 1, :] / joined[i:i + 1, i:i + 1]
            column = joined[:, i:i + 1]
            joined = jnp.where(row16 == i, pivot_row, joined - column * pivot_row)
        return mm(pick, joined, NT)

    def step(i, carry):
        first = i == 0
        par = 0
        ag = []
        gather_start(par, zv[...], ag)
        yy = jnp.where(first, 0.0, wv[...] - mm(at_small[0:16, :], zv[...]))
        qq = qv[...]
        ax = reduce_first(par, sums_of(yy, qq))
        gather_start(par, None, ag)
        ay = reduce_second(par)
        gather_parts(par, ag, 0)
        gather_parts(par, ag, 1)
        az = reduce_third(par)
        gather_parts(par, ag, 2)
        rs = products(par)
        total = reduce_finish(par)
        omega = jnp.where(first, 1.0, omega_of(total))
        beta_t = jnp.where(first, 0.0, -mm(total[:, 0:16], at_small[16:32, :]))
        alpha_t = at_small[0:16, :]
        xv[...] = xv[...] + mm(alpha_t, pv[...]) + omega * qq
        res = qq - omega * yy
        new_p = res + mm(beta_t, pv[...] - omega * sv[...])
        kept = mm(beta_t, sv[...] - omega * zv[...])
        left = yy - omega * tv[...]
        drain(ag + ax + ay + az + rs)
        vv[...] = scatter_finish(par, zv[...])
        w_new = jnp.where(first, vv[...], left + omega * mm(alpha_t, vv[...]))
        par = 1
        ag = []
        gather_start(par, w_new, ag)
        s_new = w_new + kept
        d = mm(sh[...], jnp.concatenate([s_new, res, pad96], axis=0), NT)
        ax = reduce_first(par, d)
        gather_start(par, None, ag)
        wv[...] = w_new
        pv[...] = new_p
        sv[...] = s_new
        ay = reduce_second(par)
        gather_parts(par, ag, 0)
        gather_parts(par, ag, 1)
        az = reduce_third(par)
        gather_parts(par, ag, 2)
        rs = products(par)
        total = reduce_finish(par)
        at_small[...] = solve(total)
        qv[...] = res - mm(at_small[0:16, :], s_new)
        u = mm(beta_t, zv[...] - omega * vv[...])
        drain(ag + ax + ay + az + rs)
        t_new = scatter_finish(par, w_new)
        tv[...] = t_new
        zv[...] = jnp.where(first, t_new, t_new + u)
        return carry

    lax.fori_loop(0, ITERS, step, 0)

    par = 0
    qq = qv[...]
    yy = wv[...] - mm(at_small[0:16, :], zv[...])
    ax = reduce_first(par, sums_of(yy, qq))
    partial = xv[...] + mm(at_small[0:16, :], pv[...])
    ay = reduce_second(par)
    az = reduce_third(par)
    total = reduce_finish(par)
    out_ref[...] = partial + omega_of(total) * qq
    drain(ax + ay + az)


def per_device(sizes, rhs, diagonal, blocks, block_cols, counts):
    nz, ny = sizes
    vm = pl.BlockSpec(memory_space=pltpu.VMEM)
    hbm = pl.BlockSpec(memory_space=pl.ANY)
    sm = pl.BlockSpec(memory_space=pltpu.SMEM)
    vec = pltpu.VMEM((16, 256), F32)
    dma = pltpu.SemaphoreType.DMA
    out = pl.pallas_call(
        functools.partial(kernel, sizes),
        out_shape=jax.ShapeDtypeStruct((16, 256), F32),
        in_specs=[sm, sm, hbm, hbm, hbm],
        out_specs=vm,
        scratch_shapes=[
            vec,
            pltpu.VMEM((1, 256), F32),
            pltpu.VMEM((16, 2, 128, 128), F32),
            pltpu.VMEM((16, 256, 256), BF16),
            pltpu.VMEM((8 * nz, 16, 128), F32),
            pltpu.VMEM((8 * nz, 16, 128), F32),
            pltpu.VMEM((2 * ny, 2, 16, 128), F32),
            pltpu.VMEM((2, 2 * ny, 2, 16, 128), F32),
            pltpu.VMEM((2, 4 * ny, 16, 128), F32),
            pltpu.VMEM((2, 2, 16, 128), F32),
            pltpu.VMEM((2, nz, 16, 128), F32),
            vec, vec, vec, vec, vec, vec, vec, vec, vec, vec,
            pltpu.VMEM((32, 16), F32),
            dma((2,)), dma((4,)),
            dma((40,)), dma((2, 4 * nz)), dma((2,)),
            dma((2 * ny - 1,)), dma((2, 2 * ny)),
            dma((4 * ny - 1,)), dma((2, 4 * ny)),
            dma((1,)), dma((2, 2)),
            dma((nz - 1,)), dma((2, nz)),
        ],
        compiler_params=pltpu.CompilerParams(
            collective_id=0, has_side_effects=True, vmem_limit_bytes=60 * 1024 * 1024
        ),
    )(
        block_cols.T,
        counts.reshape(-1),
        rhs.T,
        diagonal.reshape(1, -1),
        blocks,
    )
    return out.T


def solution(mesh):
    sizes = (mesh.shape["rows"] // 4, mesh.shape["cols"] // 2)
    in_specs = (
        P(("rows", "cols"), None),
        P(("rows", "cols")),
        P("rows", "cols", None, None),
        P("rows", "cols"),
        P("rows", "cols"),
    )
    return jax.shard_map(
        functools.partial(per_device, sizes),
        mesh=mesh,
        in_specs=in_specs,
        out_specs=P(("rows", "cols"), None),
        check_vma=False,
    )
```

```python
import functools

import jax
import jax.numpy as jnp
from jax import lax
from jax.experimental import pallas as pl
from jax.experimental.pallas import tpu as pltpu
from jax.sharding import PartitionSpec as P

ITERS = 4
MESH = pl.DeviceIdType.MESH
HIGHEST = lax.Precision.HIGHEST
F32 = jnp.float32
BF16 = jnp.bfloat16
NT = (((1,), (1,)), ((), ()))
NN = (((1,), (0,)), ((), ()))


def mm(a, b, dims=NN):
    return lax.dot_general(a, b, dims, precision=HIGHEST, preferred_element_type=F32)


def kernel(
    sizes,
    cols_ref, counts_ref, rhs_hbm, diag_hbm, blocks_hbm, out_ref,
    rhs_ref, diag_ref, blocks_ref, at, gb0, gb1, prod, rsb, arx, ary, arz,
    sh, pv, sv, zv, vv, rv, wv, tv, qv, xv, at_small,
    in_sem, blk_sem, ag_ssem, ag_rsem, fw_rsem, rs_ssem, rs_rsem,
    ax_ssem, ax_rsem, ay_ssem, ay_rsem, az_ssem, az_rsem,
):
    NZ, NY = sizes
    r = lax.axis_index("rows")
    c = lax.axis_index("cols")
    core = lax.rem(r, 2)
    z = lax.rem(lax.div(r, 2), NZ)
    a = lax.div(r, 2 * NZ)
    xh = lax.div(c, NY)
    y = lax.rem(c, NY)
    x = xh * 2 + a
    n_cols = 2 * NY

    rhs_in = pltpu.make_async_copy(rhs_hbm, rhs_ref, in_sem.at[0])
    diag_in = pltpu.make_async_copy(diag_hbm, diag_ref, in_sem.at[1])
    blocks_in = [
        pltpu.make_async_copy(
            blocks_hbm.at[pl.ds(4 * q, 4)], blocks_ref.at[pl.ds(4 * q, 4)], blk_sem.at[q]
        )
        for q in range(4)
    ]
    rhs_in.start()
    diag_in.start()
    for cp in blocks_in:
        cp.start()

    def device(fx, dy, dz, fk):
        xh_ = (1 - xh) if fx & 2 else xh
        a_ = (1 - a) if fx & 1 else a
        k_ = (1 - core) if fk else core
        y_ = lax.rem(y + dy, NY) if dy else y
        z_ = lax.rem(z + dz, NZ) if dz else z
        return ((a_ * NZ + z_) * 2 + k_, xh_ * NY + y_)

    def slot(fk, fa, dz):
        return ((fk * 2 + fa) * NZ + dz) * 2

    def far(n):
        return lambda d: -min(d, n - d)

    z_order = sorted(range(1, NZ), key=far(NZ))
    y_order = sorted(range(NY), key=far(NY))
    far_z = [d for d in z_order if min(d, NZ - d) >= 4]
    mid_z = [d for d in z_order if min(d, NZ - d) < 4]
    scatter_peers = [(2, dy, 0, 0) for dy in y_order] + [(0, dy, 0, 0) for dy in y_order if dy]
    chip_peers = [(0, 0, 0, 1)]
    plane_peers = [(fx, dy, 0, 1) for fx in (2, 3, 1, 0) for dy in y_order if (fx, dy) != (0, 0)]
    z_peers = [(0, 0, dz, 1) for dz in z_order]
    gather_peers = [(0, 0, dz, 1) for dz in z_order] + [(1, 0, dz, 1) for dz in mid_z]
    gather_peers += [(1, 0, 0, 1), (1, 0, 0, 0), (0, 0, 0, 1)]

    barrier = pltpu.get_barrier_semaphore()
    greet = sorted(set(scatter_peers + plane_peers + z_peers + gather_peers))
    for peer in greet:
        pl.semaphore_signal(barrier, inc=1, device_id=device(*peer), device_id_type=MESH)

    def prepare():
        for q in range(4):
            blocks_in[q].wait()

            def some(p, carry):
                for b_ in range(2):
                    b = 4 * q + 2 * p + b_
                    cnt = counts_ref[b]
                    for k in range(2):
                        blk = blocks_ref[b, k]
                        blk = jnp.where(k < cnt, blk, 0.0).T
                        hi = blk.astype(BF16)
                        mid = (blk - hi.astype(F32)).astype(BF16)
                        at[b, k * 128:(k + 1) * 128, 0:128] = hi
                        at[b, k * 128:(k + 1) * 128, 128:256] = mid
                return carry

            lax.fori_loop(0, 2, some, 0)

    rhs_in.wait()
    diag_in.wait()
    rhs = rhs_ref[...]
    sh[...] = rhs
    rv[...] = rhs
    wv[...] = rhs
    zv[...] = rhs
    qv[...] = rhs
    xv[...] = -rhs
    zero = jnp.zeros_like(rhs)
    pv[...] = zero
    sv[...] = zero
    vv[...] = zero
    tv[...] = zero
    row16 = lax.broadcasted_iota(jnp.int32, (16, 128), 0)
    lane16 = lax.broadcasted_iota(jnp.int32, (16, 128), 1)
    eye_at_32 = jnp.where(lane16 == row16 + 32, 1.0, 0.0)
    row32 = lax.broadcasted_iota(jnp.int32, (32, 128), 0)
    lane32 = lax.broadcasted_iota(jnp.int32, (32, 128), 1)
    pick = jnp.where(lane32 == row32 + 16, 1.0, 0.0)
    pad96 = jnp.zeros((96, 256), F32)
    pad112 = jnp.zeros((112, 256), F32)
    at_small[...] = jnp.zeros((32, 16), F32)

    prepare()
    pl.semaphore_wait(barrier, len(greet))

    gbs = (gb0, gb1)

    def arrival(ref, sem):
        pltpu.make_async_remote_copy(
            src_ref=ref, dst_ref=ref, send_sem=ag_ssem.at[0], recv_sem=sem,
            device_id=device(0, 0, 0, 1), device_id_type=MESH,
        ).wait_recv()

    def gather_send(par, sends, src, dst, peer, sem):
        cp = pltpu.make_async_remote_copy(
            src_ref=src, dst_ref=dst, send_sem=ag_ssem.at[len(sends)], recv_sem=sem,
            device_id=device(*peer), device_id_type=MESH,
        )
        cp.start()
        sends.append(cp)

    def gather_start(par, vec, sends):
        gb = gbs[par]
        if vec is not None:
            gb[0] = vec[:, 0:128]
            gb[1] = vec[:, 128:256]
        own = gb.at[pl.ds(0, 2)]

        def send(fk, fa, dz):
            s = slot(fk, fa, (NZ - dz) % NZ)
            gather_send(
                par, sends, own, gb.at[pl.ds(s, 2)], (fa, 0, dz, fk), ag_rsem.at[par, s // 2]
            )

        if vec is not None:
            for dz in far_z:
                send(1, 0, dz)
            for dz in mid_z[:2]:
                for fa in (1, 0):
                    send(1, fa, dz)
            send(1, 0, 0)
            return
        for dz in mid_z[2:]:
            for fa in (1, 0):
                send(1, fa, dz)
        send(1, 1, 0)
        send(0, 1, 0)

    def gather_parts(par, sends, part):
        gb = gbs[par]

        def place(fk, fa, dz, n=1):
            return gb.at[pl.ds(slot(fk, fa, dz), 2 * n)]

        def sem(fk, fa, dz):
            return ag_rsem.at[par, slot(fk, fa, dz) // 2]

        lo, n_far = min(far_z), len(far_z)
        for d in far_z if part == 0 else ():
            dz = NZ - d
            arrival(place(1, 0, dz), sem(1, 0, dz))
            gather_send(par, sends, place(1, 0, dz), place(1, 1, dz), (1, 0, 0, 0), sem(1, 1, dz))
            gather_send(par, sends, place(1, 0, dz), place(0, 1, dz), (1, 0, 0, 1), sem(0, 1, dz))
        if part == 0:
            gather_send(
                par, sends, place(1, 0, lo, n_far), place(0, 0, lo, n_far),
                (0, 0, 0, 1), fw_rsem.at[par]
            )
        for d in mid_z if part == 1 else ():
            dz = NZ - d
            for fa in (0, 1):
                arrival(place(1, fa, dz), sem(1, fa, dz))
                gather_send(
                    par, sends, place(1, fa, dz), place(0, fa, dz), (0, 0, 0, 1), sem(0, fa, dz)
                )
        if part < 2:
            return
        arrival(place(1, 0, 0), sem(1, 0, 0))
        arrival(place(1, 1, 0), sem(1, 1, 0))
        arrival(place(0, 1, 0), sem(0, 1, 0))
        arrival(place(0, 0, lo, n_far), fw_rsem.at[par])
        for d in mid_z:
            dz = NZ - d
            for fa in (0, 1):
                arrival(place(0, fa, dz), sem(0, fa, dz))
        for d in far_z:
            dz = NZ - d
            arrival(place(1, 1, dz), sem(1, 1, dz))
            arrival(place(0, 1, dz), sem(0, 1, dz))

    def block_row(gb, b):
        parts = []
        for k in range(2):
            l = cols_ref[k, b]
            fk = ((l >> 1) & 1) ^ core
            dz = ((l >> 2) + NZ - z) & (NZ - 1)
            fa = (l // (4 * NZ)) ^ a
            parts.append(gb[slot(fk, fa, dz) + (l & 1)])
        v = jnp.concatenate(parts, axis=1)
        vh = v.astype(BF16)
        vm = (v - vh.astype(F32)).astype(BF16)
        both = jnp.concatenate([vh, vm], axis=0)
        full = lax.dot_general(both, at[b], NN, preferred_element_type=F32)
        return full[0:16, 0:128] + (full[16:32, 0:128] + full[0:16, 128:256])

    def products(par):
        gb = gbs[par]
        sends = []
        for n, peer in enumerate(scatter_peers + [(0, 0, 0, 0)]):
            c_ = device(*peer)[1]
            for h in range(2):
                prod[c_, h] = block_row(gb, c_ * 2 + h)
            if n < len(scatter_peers):
                cp = pltpu.make_async_remote_copy(
                    src_ref=prod.at[c_],
                    dst_ref=rsb.at[par, c],
                    send_sem=rs_ssem.at[n],
                    recv_sem=rs_rsem.at[par, c],
                    device_id=device(*peer),
                    device_id_type=MESH,
                )
                cp.start()
                sends.append(cp)
        return sends

    def scatter_finish(par, vec):
        own = prod[c]
        total = jnp.concatenate([own[0], own[1]], axis=1) + diag_ref[...] * vec
        for peer in reversed(scatter_peers):
            c_ = device(*peer)[1]
            pltpu.make_async_remote_copy(
                src_ref=prod.at[c_],
                dst_ref=rsb.at[par, c_],
                send_sem=rs_ssem.at[0],
                recv_sem=rs_rsem.at[par, c_],
                device_id=device(*peer),
                device_id_type=MESH,
            ).wait_recv()
            got = rsb[par, c_]
            total = total + jnp.concatenate([got[0], got[1]], axis=1)
        return total

    def spread(par, part, buf, mine, peers, ssem, rsem):
        rows = part.shape[0]
        buf[par, mine, 0:rows] = part
        sends = []
        for n, peer in enumerate(peers):
            cp = pltpu.make_async_remote_copy(
                src_ref=buf.at[par, mine, pl.ds(0, rows)], dst_ref=buf.at[par, mine, pl.ds(0, rows)],
                send_sem=ssem.at[n], recv_sem=rsem.at[par, mine],
                device_id=device(*peer), device_id_type=MESH,
            )
            cp.start()
            sends.append(cp)
        return sends

    def collect(par, rows, buf, index_of, peers, ssem, rsem):
        for peer in reversed(peers):
            there = index_of(*device(*peer))
            pltpu.make_async_remote_copy(
                src_ref=buf.at[par, there, pl.ds(0, rows)], dst_ref=buf.at[par, there, pl.ds(0, rows)],
                send_sem=ssem.at[0], recv_sem=rsem.at[par, there],
                device_id=device(*peer), device_id_type=MESH,
            ).wait_recv()
        parts = [buf[par, n, 0:rows] for n in range(buf.shape[1])]
        while len(parts) > 1:
            parts = [parts[n] + parts[n + 1] for n in range(0, len(parts), 2)]
        return parts[0]

    def chip_index(r_, c_):
        return lax.rem(r_, 2)

    def plane_index(r_, c_):
        return (lax.div(c_, NY) * 2 + lax.div(r_, 2 * NZ)) * NY + lax.rem(c_, NY)

    def z_index(r_, c_):
        return lax.rem(lax.div(r_, 2), NZ)

    in_plane = (arx, plane_index, plane_peers, ax_ssem, ax_rsem)
    in_chip = (ary, chip_index, chip_peers, ay_ssem, ay_rsem)
    in_z = (arz, z_index, z_peers, az_ssem, az_rsem)

    def reduce_first(par, part):
        buf, index_of, peers, ssem, rsem = in_chip
        return spread(par, part, buf, index_of(r, c), peers, ssem, rsem)

    def reduce_second(par, rows=16):
        part = collect(par, rows, *in_chip)
        buf, index_of, peers, ssem, rsem = in_plane
        return spread(par, part, buf, index_of(r, c), peers, ssem, rsem)

    def reduce_third(par, rows=16):
        part = collect(par, rows, *in_plane)
        buf, index_of, peers, ssem, rsem = in_z
        return spread(par, part, buf, index_of(r, c), peers, ssem, rsem)

    def reduce_finish(par, rows=16):
        return collect(par, rows, *in_z)

    def drain(sends):
        for cp in sends:
            cp.wait_send()

    def omega_part():
        yy = wv[...] - mm(at_small[0:16, :], zv[...])
        return yy

    def sums_of(yy, qq):
        d = mm(yy, jnp.concatenate([sh[...], pad112], axis=0), NT)
        along = jnp.sum(yy * qq, axis=1, keepdims=True)
        square = jnp.sum(yy * yy, axis=1, keepdims=True)
        return jnp.where(lane16 == 16, along, jnp.where(lane16 == 17, square, d))

    def omega_of(total):
        lane = lane16[0:total.shape[0], :]
        along = jnp.sum(jnp.where(lane == 16, total, 0.0), keepdims=True)
        square = jnp.sum(jnp.where(lane == 17, total, 0.0), keepdims=True)
        return along / square

    def solve(total):
        joined = jnp.where(lane16 < 32, total, eye_at_32)
        for i in range(16):
            pivot_row = joined[i:i + 1, :] / joined[i:i + 1, i:i + 1]
            column = joined[:, i:i + 1]
            joined = jnp.where(row16 == i, pivot_row, joined - column * pivot_row)
        return mm(pick, joined, NT)

    def step(i, carry):
        first = i == 0
        par = 0
        ag = []
        gather_start(par, zv[...], ag)
        yy = jnp.where(first, 0.0, wv[...] - mm(at_small[0:16, :], zv[...]))
        qq = qv[...]
        ax = reduce_first(par, sums_of(yy, qq))
        gather_start(par, None, ag)
        ay = reduce_second(par)
        gather_parts(par, ag, 0)
        gather_parts(par, ag, 1)
        az = reduce_third(par)
        gather_parts(par, ag, 2)
        rs = products(par)
        total = reduce_finish(par)
        omega = jnp.where(first, 1.0, omega_of(total))
        beta_t = jnp.where(first, 0.0, -mm(total[:, 0:16], at_small[16:32, :]))
        alpha_t = at_small[0:16, :]
        xv[...] = xv[...] + mm(alpha_t, pv[...]) + omega * qq
        res = qq - omega * yy
        new_p = res + mm(beta_t, pv[...] - omega * sv[...])
        kept = mm(beta_t, sv[...] - omega * zv[...])
        left = yy - omega * tv[...]
        drain(ag + ax + ay + az + rs)
        vv[...] = scatter_finish(par, zv[...])
        w_new = jnp.where(first, vv[...], left + mm(omega * alpha_t, vv[...]))
        par = 1
        ag = []
        gather_start(par, w_new, ag)
        s_new = w_new + kept
        d = mm(sh[...], jnp.concatenate([s_new, res, pad96], axis=0), NT)
        ax = reduce_first(par, d)
        gather_start(par, None, ag)
        wv[...] = w_new
        pv[...] = new_p
        sv[...] = s_new
        ay = reduce_second(par)
        gather_parts(par, ag, 0)
        gather_parts(par, ag, 1)
        az = reduce_third(par)
        gather_parts(par, ag, 2)
        rs = products(par)
        total = reduce_finish(par)
        at_small[...] = solve(total)
        qv[...] = res - mm(at_small[0:16, :], s_new)
        u = mm(beta_t, zv[...] - omega * vv[...])
        drain(ag + ax + ay + az + rs)
        t_new = scatter_finish(par, w_new)
        tv[...] = t_new
        zv[...] = jnp.where(first, t_new, t_new + u)
        return carry

    lax.fori_loop(0, ITERS, step, 0)

    par = 0
    qq = qv[...]
    yy = wv[...] - mm(at_small[0:16, :], zv[...])

    def eight(product):
        folded = product[:, 0:128] + product[:, 128:256]
        return jnp.sum(folded[0:8, :] + folded[8:16, :], axis=1, keepdims=True)

    lane8 = lane16[0:8, :]
    part = jnp.where(lane8 == 16, eight(yy * qq), jnp.where(lane8 == 17, eight(yy * yy), 0.0))
    ax = reduce_first(par, part)
    partial = xv[...] + mm(at_small[0:16, :], pv[...])
    ay = reduce_second(par, 8)
    az = reduce_third(par, 8)
    total = reduce_finish(par, 8)
    out_ref[...] = partial + omega_of(total) * qq
    drain(ax + ay + az)


def per_device(sizes, rhs, diagonal, blocks, block_cols, counts):
    nz, ny = sizes
    vm = pl.BlockSpec(memory_space=pltpu.VMEM)
    hbm = pl.BlockSpec(memory_space=pl.ANY)
    sm = pl.BlockSpec(memory_space=pltpu.SMEM)
    vec = pltpu.VMEM((16, 256), F32)
    dma = pltpu.SemaphoreType.DMA
    out = pl.pallas_call(
        functools.partial(kernel, sizes),
        out_shape=jax.ShapeDtypeStruct((16, 256), F32),
        in_specs=[sm, sm, hbm, hbm, hbm],
        out_specs=vm,
        scratch_shapes=[
            vec,
            pltpu.VMEM((1, 256), F32),
            pltpu.VMEM((16, 2, 128, 128), F32),
            pltpu.VMEM((16, 256, 256), BF16),
            pltpu.VMEM((8 * nz, 16, 128), F32),
            pltpu.VMEM((8 * nz, 16, 128), F32),
            pltpu.VMEM((2 * ny, 2, 16, 128), F32),
            pltpu.VMEM((2, 2 * ny, 2, 16, 128), F32),
            pltpu.VMEM((2, 4 * ny, 16, 128), F32),
            pltpu.VMEM((2, 2, 16, 128), F32),
            pltpu.VMEM((2, nz, 16, 128), F32),
            vec, vec, vec, vec, vec, vec, vec, vec, vec, vec,
            pltpu.VMEM((32, 16), F32),
            dma((2,)), dma((4,)),
            dma((40,)), dma((2, 4 * nz)), dma((2,)),
            dma((2 * ny - 1,)), dma((2, 2 * ny)),
            dma((4 * ny - 1,)), dma((2, 4 * ny)),
            dma((1,)), dma((2, 2)),
            dma((nz - 1,)), dma((2, nz)),
        ],
        compiler_params=pltpu.CompilerParams(
            collective_id=0, has_side_effects=True, vmem_limit_bytes=60 * 1024 * 1024
        ),
    )(
        block_cols.T,
        counts.reshape(-1),
        rhs.T,
        diagonal.reshape(1, -1),
        blocks,
    )
    return out.T


def solution(mesh):
    sizes = (mesh.shape["rows"] // 4, mesh.shape["cols"] // 2)
    in_specs = (
        P(("rows", "cols"), None),
        P(("rows", "cols")),
        P("rows", "cols", None, None),
        P("rows", "cols"),
        P("rows", "cols"),
    )
    return jax.shard_map(
        functools.partial(per_device, sizes),
        mesh=mesh,
        in_specs=in_specs,
        out_specs=P(("rows", "cols"), None),
        check_vma=False,
    )
```

```python
import functools

import jax
import jax.numpy as jnp
from jax import lax
from jax.experimental import pallas as pl
from jax.experimental.pallas import tpu as pltpu
from jax.sharding import PartitionSpec as P

ITERS = 4
MESH = pl.DeviceIdType.MESH
HIGHEST = lax.Precision.HIGHEST
F32 = jnp.float32
BF16 = jnp.bfloat16
NT = (((1,), (1,)), ((), ()))
NN = (((1,), (0,)), ((), ()))


def mm(a, b, dims=NN):
    return lax.dot_general(a, b, dims, precision=HIGHEST, preferred_element_type=F32)


def kernel(
    sizes,
    cols_ref, counts_ref, rhs_hbm, diag_hbm, blocks_hbm, out_ref,
    rhs_ref, diag_ref, blocks_ref, at, gb0, gb1, prod, rsb, arx, ary, arz,
    sh, pv, sv, zv, vv, rv, wv, tv, qv, xv, at_small,
    in_sem, blk_sem, ag_ssem, ag_rsem, fw_rsem, rs_ssem, rs_rsem,
    ax_ssem, ax_rsem, ay_ssem, ay_rsem, az_ssem, az_rsem,
):
    NZ, NY = sizes
    r = lax.axis_index("rows")
    c = lax.axis_index("cols")
    core = lax.rem(r, 2)
    z = lax.rem(lax.div(r, 2), NZ)
    a = lax.div(r, 2 * NZ)
    xh = lax.div(c, NY)
    y = lax.rem(c, NY)
    x = xh * 2 + a
    n_cols = 2 * NY

    rhs_in = pltpu.make_async_copy(rhs_hbm, rhs_ref, in_sem.at[0])
    diag_in = pltpu.make_async_copy(diag_hbm, diag_ref, in_sem.at[1])
    blocks_in = [
        pltpu.make_async_copy(
            blocks_hbm.at[pl.ds(4 * q, 4)], blocks_ref.at[pl.ds(4 * q, 4)], blk_sem.at[q]
        )
        for q in range(4)
    ]
    rhs_in.start()
    diag_in.start()
    for cp in blocks_in:
        cp.start()

    def device(fx, dy, dz, fk):
        xh_ = (1 - xh) if fx & 2 else xh
        a_ = (1 - a) if fx & 1 else a
        k_ = (1 - core) if fk else core
        y_ = lax.rem(y + dy, NY) if dy else y
        z_ = lax.rem(z + dz, NZ) if dz else z
        return ((a_ * NZ + z_) * 2 + k_, xh_ * NY + y_)

    def slot(fk, fa, dz):
        return ((fk * 2 + fa) * NZ + dz) * 2

    def far(n):
        return lambda d: -min(d, n - d)

    z_order = sorted(range(1, NZ), key=far(NZ))
    y_order = sorted(range(NY), key=far(NY))
    far_z = [d for d in z_order if min(d, NZ - d) >= 4]
    mid_z = [d for d in z_order if min(d, NZ - d) < 4]
    scatter_peers = [(2, dy, 0, 0) for dy in y_order] + [(0, dy, 0, 0) for dy in y_order if dy]
    chip_peers = [(0, 0, 0, 1)]
    plane_peers = [(fx, dy, 0, 1) for fx in (2, 3, 1, 0) for dy in y_order if (fx, dy) != (0, 0)]
    z_peers = [(0, 0, dz, 1) for dz in z_order]
    gather_peers = [(0, 0, dz, 1) for dz in z_order] + [(1, 0, dz, 1) for dz in mid_z]
    gather_peers += [(1, 0, 0, 1), (1, 0, 0, 0), (0, 0, 0, 1)]

    barrier = pltpu.get_barrier_semaphore()
    greet = sorted(set(scatter_peers + plane_peers + z_peers + gather_peers))
    for peer in greet:
        pl.semaphore_signal(barrier, inc=1, device_id=device(*peer), device_id_type=MESH)

    def prepare():
        for q in range(4):
            blocks_in[q].wait()

            def some(p, carry):
                for b_ in range(2):
                    b = 4 * q + 2 * p + b_
                    cnt = counts_ref[b]
                    for k in range(2):
                        blk = blocks_ref[b, k]
                        blk = jnp.where(k < cnt, blk, 0.0).T
                        hi = blk.astype(BF16)
                        mid = (blk - hi.astype(F32)).astype(BF16)
                        at[b, k * 128:(k + 1) * 128, 0:128] = hi
                        at[b, k * 128:(k + 1) * 128, 128:256] = mid
                return carry

            lax.fori_loop(0, 2, some, 0)

    rhs_in.wait()
    diag_in.wait()
    rhs = rhs_ref[...]
    sh[...] = rhs
    rv[...] = rhs
    wv[...] = rhs
    zv[...] = rhs
    qv[...] = rhs
    xv[...] = -rhs
    zero = jnp.zeros_like(rhs)
    pv[...] = zero
    sv[...] = zero
    vv[...] = zero
    tv[...] = zero
    row16 = lax.broadcasted_iota(jnp.int32, (16, 128), 0)
    lane16 = lax.broadcasted_iota(jnp.int32, (16, 128), 1)
    eye_at_32 = jnp.where(lane16 == row16 + 32, 1.0, 0.0)
    row32 = lax.broadcasted_iota(jnp.int32, (32, 128), 0)
    lane32 = lax.broadcasted_iota(jnp.int32, (32, 128), 1)
    pick = jnp.where(lane32 == row32 + 16, 1.0, 0.0)
    pad96 = jnp.zeros((96, 256), F32)
    pad112 = jnp.zeros((112, 256), F32)
    at_small[...] = jnp.zeros((32, 16), F32)

    prepare()
    pl.semaphore_wait(barrier, len(greet))

    gbs = (gb0, gb1)

    def arrival(ref, sem):
        pltpu.make_async_remote_copy(
            src_ref=ref, dst_ref=ref, send_sem=ag_ssem.at[0], recv_sem=sem,
            device_id=device(0, 0, 0, 1), device_id_type=MESH,
        ).wait_recv()

    def gather_send(par, sends, src, dst, peer, sem):
        cp = pltpu.make_async_remote_copy(
            src_ref=src, dst_ref=dst, send_sem=ag_ssem.at[len(sends)], recv_sem=sem,
            device_id=device(*peer), device_id_type=MESH,
        )
        cp.start()
        sends.append(cp)

    def gather_start(par, vec, sends):
        gb = gbs[par]
        if vec is not None:
            gb[0] = vec[:, 0:128]
            gb[1] = vec[:, 128:256]
        own = gb.at[pl.ds(0, 2)]

        def send(fk, fa, dz):
            s = slot(fk, fa, (NZ - dz) % NZ)
            gather_send(
                par, sends, own, gb.at[pl.ds(s, 2)], (fa, 0, dz, fk), ag_rsem.at[par, s // 2]
            )

        if vec is not None:
            for dz in far_z:
                send(1, 0, dz)
            for dz in mid_z[:2]:
                for fa in (1, 0):
                    send(1, fa, dz)
            send(1, 0, 0)
            return
        for dz in mid_z[2:]:
            for fa in (1, 0):
                send(1, fa, dz)
        send(1, 1, 0)
        send(0, 1, 0)

    def gather_parts(par, sends, part):
        gb = gbs[par]

        def place(fk, fa, dz, n=1):
            return gb.at[pl.ds(slot(fk, fa, dz), 2 * n)]

        def sem(fk, fa, dz):
            return ag_rsem.at[par, slot(fk, fa, dz) // 2]

        lo, n_far = min(far_z), len(far_z)
        for d in far_z if part == 0 else ():
            dz = NZ - d
            arrival(place(1, 0, dz), sem(1, 0, dz))
            gather_send(par, sends, place(1, 0, dz), place(1, 1, dz), (1, 0, 0, 0), sem(1, 1, dz))
            gather_send(par, sends, place(1, 0, dz), place(0, 1, dz), (1, 0, 0, 1), sem(0, 1, dz))
        if part == 0:
            gather_send(
                par, sends, place(1, 0, lo, n_far), place(0, 0, lo, n_far),
                (0, 0, 0, 1), fw_rsem.at[par]
            )
        for d in mid_z if part == 1 else ():
            dz = NZ - d
            for fa in (0, 1):
                arrival(place(1, fa, dz), sem(1, fa, dz))
                gather_send(
                    par, sends, place(1, fa, dz), place(0, fa, dz), (0, 0, 0, 1), sem(0, fa, dz)
                )
        if part < 2:
            return
        arrival(place(1, 0, 0), sem(1, 0, 0))
        arrival(place(1, 1, 0), sem(1, 1, 0))
        arrival(place(0, 1, 0), sem(0, 1, 0))
        arrival(place(0, 0, lo, n_far), fw_rsem.at[par])
        for d in mid_z:
            dz = NZ - d
            for fa in (0, 1):
                arrival(place(0, fa, dz), sem(0, fa, dz))
        for d in far_z:
            dz = NZ - d
            arrival(place(1, 1, dz), sem(1, 1, dz))
            arrival(place(0, 1, dz), sem(0, 1, dz))

    def block_row(gb, b):
        parts = []
        for k in range(2):
            l = cols_ref[k, b]
            fk = ((l >> 1) & 1) ^ core
            dz = ((l >> 2) + NZ - z) & (NZ - 1)
            fa = (l // (4 * NZ)) ^ a
            parts.append(gb[slot(fk, fa, dz) + (l & 1)])
        v = jnp.concatenate(parts, axis=1)
        vh = v.astype(BF16)
        vm = (v - vh.astype(F32)).astype(BF16)
        both = jnp.concatenate([vh, vm], axis=0)
        full = lax.dot_general(both, at[b], NN, preferred_element_type=F32)
        return full[0:16, 0:128] + (full[16:32, 0:128] + full[0:16, 128:256])

    def products(par):
        gb = gbs[par]
        sends = []
        for n, peer in enumerate(scatter_peers + [(0, 0, 0, 0)]):
            c_ = device(*peer)[1]
            for h in range(2):
                prod[c_, h] = block_row(gb, c_ * 2 + h)
            if n < len(scatter_peers):
                cp = pltpu.make_async_remote_copy(
                    src_ref=prod.at[c_],
                    dst_ref=rsb.at[par, c],
                    send_sem=rs_ssem.at[n],
                    recv_sem=rs_rsem.at[par, c],
                    device_id=device(*peer),
                    device_id_type=MESH,
                )
                cp.start()
                sends.append(cp)
        return sends

    def scatter_finish(par, vec):
        own = prod[c]
        total = jnp.concatenate([own[0], own[1]], axis=1) + diag_ref[...] * vec
        for peer in reversed(scatter_peers):
            c_ = device(*peer)[1]
            pltpu.make_async_remote_copy(
                src_ref=prod.at[c_],
                dst_ref=rsb.at[par, c_],
                send_sem=rs_ssem.at[0],
                recv_sem=rs_rsem.at[par, c_],
                device_id=device(*peer),
                device_id_type=MESH,
            ).wait_recv()
            got = rsb[par, c_]
            total = total + jnp.concatenate([got[0], got[1]], axis=1)
        return total

    def spread(par, part, buf, mine, peers, ssem, rsem):
        rows = part.shape[0]
        buf[par, mine, 0:rows] = part
        sends = []
        for n, peer in enumerate(peers):
            cp = pltpu.make_async_remote_copy(
                src_ref=buf.at[par, mine, pl.ds(0, rows)], dst_ref=buf.at[par, mine, pl.ds(0, rows)],
                send_sem=ssem.at[n], recv_sem=rsem.at[par, mine],
                device_id=device(*peer), device_id_type=MESH,
            )
            cp.start()
            sends.append(cp)
        return sends

    def collect(par, rows, buf, index_of, peers, ssem, rsem):
        for peer in reversed(peers):
            there = index_of(*device(*peer))
            pltpu.make_async_remote_copy(
                src_ref=buf.at[par, there, pl.ds(0, rows)], dst_ref=buf.at[par, there, pl.ds(0, rows)],
                send_sem=ssem.at[0], recv_sem=rsem.at[par, there],
                device_id=device(*peer), device_id_type=MESH,
            ).wait_recv()
        parts = [buf[par, n, 0:rows] for n in range(buf.shape[1])]
        while len(parts) > 1:
            parts = [parts[n] + parts[n + 1] for n in range(0, len(parts), 2)]
        return parts[0]

    def chip_index(r_, c_):
        return lax.rem(r_, 2)

    def plane_index(r_, c_):
        return (lax.div(c_, NY) * 2 + lax.div(r_, 2 * NZ)) * NY + lax.rem(c_, NY)

    def z_index(r_, c_):
        return lax.rem(lax.div(r_, 2), NZ)

    in_plane = (arx, plane_index, plane_peers, ax_ssem, ax_rsem)
    in_chip = (ary, chip_index, chip_peers, ay_ssem, ay_rsem)
    in_z = (arz, z_index, z_peers, az_ssem, az_rsem)

    def packed(part):
        return part[0:8, :] + pltpu.roll(part[8:16, :], 64, 1)

    def unpacked(total):
        return jnp.concatenate([total, pltpu.roll(total, 64, 1)], axis=0)

    def reduce_first(par, part):
        buf, index_of, peers, ssem, rsem = in_chip
        return spread(par, part, buf, index_of(r, c), peers, ssem, rsem)

    def reduce_second(par, rows=16):
        part = collect(par, rows, *in_chip)
        buf, index_of, peers, ssem, rsem = in_plane
        return spread(par, part, buf, index_of(r, c), peers, ssem, rsem)

    def reduce_third(par, rows=16):
        part = collect(par, rows, *in_plane)
        buf, index_of, peers, ssem, rsem = in_z
        return spread(par, part, buf, index_of(r, c), peers, ssem, rsem)

    def reduce_finish(par, rows=16):
        return collect(par, rows, *in_z)

    def drain(sends):
        for cp in sends:
            cp.wait_send()

    def omega_part():
        yy = wv[...] - mm(at_small[0:16, :], zv[...])
        return yy

    def sums_of(yy, qq):
        d = mm(yy, jnp.concatenate([sh[...], pad112], axis=0), NT)
        along = jnp.sum(yy * qq, axis=1, keepdims=True)
        square = jnp.sum(yy * yy, axis=1, keepdims=True)
        return jnp.where(lane16 == 16, along, jnp.where(lane16 == 17, square, d))

    def omega_of(total):
        lane = lane16[0:total.shape[0], :]
        along = jnp.sum(jnp.where(lane == 16, total, 0.0), keepdims=True)
        square = jnp.sum(jnp.where(lane == 17, total, 0.0), keepdims=True)
        return along / square

    def solve(total):
        joined = jnp.where(lane16 < 32, total, eye_at_32)
        for i in range(16):
            pivot_row = joined[i:i + 1, :] / joined[i:i + 1, i:i + 1]
            column = joined[:, i:i + 1]
            joined = jnp.where(row16 == i, pivot_row, joined - column * pivot_row)
        return mm(pick, joined, NT)

    def step(i, carry):
        first = i == 0
        par = 0
        ag = []
        gather_start(par, zv[...], ag)
        yy = jnp.where(first, 0.0, wv[...] - mm(at_small[0:16, :], zv[...]))
        qq = qv[...]
        ax = reduce_first(par, packed(sums_of(yy, qq)))
        gather_start(par, None, ag)
        ay = reduce_second(par, 8)
        gather_parts(par, ag, 0)
        gather_parts(par, ag, 1)
        az = reduce_third(par, 8)
        gather_parts(par, ag, 2)
        rs = products(par)
        total = unpacked(reduce_finish(par, 8))
        omega = jnp.where(first, 1.0, omega_of(total))
        beta_t = jnp.where(first, 0.0, -mm(total[:, 0:16], at_small[16:32, :]))
        alpha_t = at_small[0:16, :]
        xv[...] = xv[...] + mm(alpha_t, pv[...]) + omega * qq
        res = qq - omega * yy
        new_p = res + mm(beta_t, pv[...] - omega * sv[...])
        kept = mm(beta_t, sv[...] - omega * zv[...])
        left = yy - omega * tv[...]
        drain(ag + ax + ay + az + rs)
        vv[...] = scatter_finish(par, zv[...])
        w_new = jnp.where(first, vv[...], left + mm(omega * alpha_t, vv[...]))
        par = 1
        ag = []
        gather_start(par, w_new, ag)
        s_new = w_new + kept
        d = mm(sh[...], jnp.concatenate([s_new, res, pad96], axis=0), NT)
        ax = reduce_first(par, packed(d))
        gather_start(par, None, ag)
        wv[...] = w_new
        pv[...] = new_p
        sv[...] = s_new
        ay = reduce_second(par, 8)
        gather_parts(par, ag, 0)
        gather_parts(par, ag, 1)
        az = reduce_third(par, 8)
        gather_parts(par, ag, 2)
        rs = products(par)
        total = unpacked(reduce_finish(par, 8))
        at_small[...] = solve(total)
        qv[...] = res - mm(at_small[0:16, :], s_new)
        u = mm(beta_t, zv[...] - omega * vv[...])
        drain(ag + ax + ay + az + rs)
        t_new = scatter_finish(par, w_new)
        tv[...] = t_new
        zv[...] = jnp.where(first, t_new, t_new + u)
        return carry

    lax.fori_loop(0, ITERS, step, 0)

    par = 0
    qq = qv[...]
    yy = wv[...] - mm(at_small[0:16, :], zv[...])

    def eight(product):
        folded = product[:, 0:128] + product[:, 128:256]
        return jnp.sum(folded[0:8, :] + folded[8:16, :], axis=1, keepdims=True)

    lane8 = lane16[0:8, :]
    part = jnp.where(lane8 == 16, eight(yy * qq), jnp.where(lane8 == 17, eight(yy * yy), 0.0))
    ax = reduce_first(par, part)
    partial = xv[...] + mm(at_small[0:16, :], pv[...])
    ay = reduce_second(par, 8)
    az = reduce_third(par, 8)
    total = reduce_finish(par, 8)
    out_ref[...] = partial + omega_of(total) * qq
    drain(ax + ay + az)


def per_device(sizes, rhs, diagonal, blocks, block_cols, counts):
    nz, ny = sizes
    vm = pl.BlockSpec(memory_space=pltpu.VMEM)
    hbm = pl.BlockSpec(memory_space=pl.ANY)
    sm = pl.BlockSpec(memory_space=pltpu.SMEM)
    vec = pltpu.VMEM((16, 256), F32)
    dma = pltpu.SemaphoreType.DMA
    out = pl.pallas_call(
        functools.partial(kernel, sizes),
        out_shape=jax.ShapeDtypeStruct((16, 256), F32),
        in_specs=[sm, sm, hbm, hbm, hbm],
        out_specs=vm,
        scratch_shapes=[
            vec,
            pltpu.VMEM((1, 256), F32),
            pltpu.VMEM((16, 2, 128, 128), F32),
            pltpu.VMEM((16, 256, 256), BF16),
            pltpu.VMEM((8 * nz, 16, 128), F32),
            pltpu.VMEM((8 * nz, 16, 128), F32),
            pltpu.VMEM((2 * ny, 2, 16, 128), F32),
            pltpu.VMEM((2, 2 * ny, 2, 16, 128), F32),
            pltpu.VMEM((2, 4 * ny, 16, 128), F32),
            pltpu.VMEM((2, 2, 16, 128), F32),
            pltpu.VMEM((2, nz, 16, 128), F32),
            vec, vec, vec, vec, vec, vec, vec, vec, vec, vec,
            pltpu.VMEM((32, 16), F32),
            dma((2,)), dma((4,)),
            dma((40,)), dma((2, 4 * nz)), dma((2,)),
            dma((2 * ny - 1,)), dma((2, 2 * ny)),
            dma((4 * ny - 1,)), dma((2, 4 * ny)),
            dma((1,)), dma((2, 2)),
            dma((nz - 1,)), dma((2, nz)),
        ],
        compiler_params=pltpu.CompilerParams(
            collective_id=0, has_side_effects=True, vmem_limit_bytes=60 * 1024 * 1024
        ),
    )(
        block_cols.T,
        counts.reshape(-1),
        rhs.T,
        diagonal.reshape(1, -1),
        blocks,
    )
    return out.T


def solution(mesh):
    sizes = (mesh.shape["rows"] // 4, mesh.shape["cols"] // 2)
    in_specs = (
        P(("rows", "cols"), None),
        P(("rows", "cols")),
        P("rows", "cols", None, None),
        P("rows", "cols"),
        P("rows", "cols"),
    )
    return jax.shard_map(
        functools.partial(per_device, sizes),
        mesh=mesh,
        in_specs=in_specs,
        out_specs=P(("rows", "cols"), None),
        check_vma=False,
    )
```
